32 devices in a mesh: dp: 8 (over z, core), tensor: 4 (over y, x).
Axes of the slice: x: 2, y: 2, z: 4, core: 2. Of those that a mesh axis runs over, the one named last changes fastest.
Arguments:
- queries: bfloat16 [3584, 8192], P('dp', 'tensor'), may hold values from -6 to 6
- features: bfloat16 [16, 384, 8192], P('dp', None, 'tensor'), may hold values from -6 to 6
- kv_weight: bfloat16 [8192, 2048], P('tensor'), may hold values from -0.0625 to 0.0625
- q_gain: float32 [128], replicated, may hold values from 0.5 to 2
- k_gain: float32 [128], replicated, may hold values from 0.5 to 2
- counts: int32 [16], replicated, may hold values from 1 to 16, as said below
- owner: int32 [16], replicated, may hold values from 0 to 15, as said below
Outputs:
- attended: bfloat16 [3584, 8192], P('dp', 'tensor')
The draws below stay inside these ranges and needn't reach their ends.
Inputs may be any that keep to these rules, and one draw needn't show every extreme that they name: `counts`: every sample has 1 to 16 images; in every draw some sample has 16 and some has one. `owner`: there are 2 different shifts c_j, each from 0 to the number of dp indices minus 1; sample s = e * 2 + j goes to slot ((e + c_j) modulo the number of dp indices) * 2 + j, with the same c_j for every e.
All inputs are finite; a program needn't handle non-finite values.
Results may differ from the reference program's by a relative error of at most 0.028.
Values may be sent and summed in bfloat16 or wider, within the bound.
A program may use at most 64 MiB of HBM per device.

```python
import math
import jax
import jax.numpy as jnp
from jax import lax

VIS = 8192
QH = 64
KVH = 8
HD = 128
TXT = 224
PATCH = 24
MAX_IMAGES = 16
SAMP_DEV = 2
SAMPLES = 16
N_TENSOR = 4


def draw_counts(key, part):
    first_key, second_key = jax.random.split(jax.random.fold_in(key, 11), 2)
    drawn = jax.random.randint(first_key, (SAMPLES,), 1, MAX_IMAGES + 1).astype(jnp.int32)
    chosen = jax.random.permutation(second_key, SAMPLES)[:2]
    drawn = drawn.at[chosen[0]].set(MAX_IMAGES)
    drawn = drawn.at[chosen[1]].set(1)
    return drawn.astype(jnp.int32)


def draw_owner(key, part):
    shard_total = SAMPLES // SAMP_DEV
    base_key = jax.random.fold_in(key, 23)
    shift_list = jax.random.permutation(base_key, shard_total).astype(jnp.int32)[:SAMP_DEV]
    encoder = jnp.arange(shard_total, dtype=jnp.int32)[:, None]
    position = jnp.arange(SAMP_DEV, dtype=jnp.int32)[None, :]
    target = (encoder + shift_list[None, :]) % shard_total
    return (target * SAMP_DEV + position).reshape(-1).astype(jnp.int32)


def shard_levels(own_key, extent, cuts, low, largest):
    factor_of = 1.0
    for dim, blocks in cuts:
        draws = jax.random.uniform(jax.random.fold_in(jax.random.fold_in(own_key, 6), dim), (blocks,), jnp.float32, low / len(cuts), largest / len(cuts))
        factor_of = factor_of * jnp.repeat(jnp.exp(draws), extent[dim] // blocks).reshape((-1,) + (1,) * (len(extent) - 1 - dim))
    return factor_of


def scatter_about(own_key, dims, deviation, most, shards=(), kind=jnp.bfloat16):
    result = deviation * jax.random.normal(own_key, dims, jnp.float32)
    if shards:
        result = result * shard_levels(own_key, dims, shards, -0.22, 0.18)
    return jnp.clip(result, -most, most).astype(kind)


def setup_inputs(seed: int = 0) -> dict:
    arg_keys = jax.random.split(jax.random.key(seed), 8)
    queries = scatter_about(arg_keys[0], (SAMPLES * TXT, QH * HD), 1.0, 6.0, ((0, 8), (1, 4)))
    features = scatter_about(arg_keys[1], (SAMPLES, MAX_IMAGES * PATCH, VIS), 1.0, 6.0, ((0, 8), (2, 4)))
    kv_weight = scatter_about(arg_keys[2], (VIS, 2 * KVH * HD), VIS ** -0.5, 0.0625, ((0, 4),))
    q_gain = jnp.clip(jnp.exp(jax.random.uniform(arg_keys[3], (HD,), jnp.float32, math.log(0.5), math.log(2.0))), 0.5, 2.0)
    k_gain = jnp.clip(jnp.exp(jax.random.uniform(arg_keys[4], (HD,), jnp.float32, math.log(0.5), math.log(2.0))), 0.5, 2.0)
    counts = draw_counts(jax.random.fold_in(arg_keys[7], 71), 0)
    owner = draw_owner(jax.random.fold_in(arg_keys[7], 71), 0)
    return {"queries": queries, "features": features, "kv_weight": kv_weight, "q_gain": q_gain, "k_gain": k_gain, "counts": counts, "owner": owner}


def normalize_rows(values_in, gain):
    return values_in * lax.rsqrt(lax.optimization_barrier(jnp.mean(values_in * values_in, axis=-1, keepdims=True)) + 1e-05) * gain

def reference(queries, features, kv_weight, q_gain, k_gain, counts, owner):
    group_size = QH // KVH
    token_count = features.shape[1]
    piece_width = VIS // N_TENSOR
    weight_groups = kv_weight.astype(jnp.float32).reshape(N_TENSOR, piece_width, 2 * KVH * HD)
    source_of = jnp.zeros((SAMPLES,), jnp.int32).at[owner].set(jnp.arange(SAMPLES, dtype=jnp.int32))
    query_blocks = queries.reshape(SAMPLES, TXT, QH, HD)

    def attend_slot(slot_id):
        sample = source_of[slot_id]
        feature_rows = features[sample].astype(jnp.float32).reshape(token_count, N_TENSOR, piece_width)
        partials = jnp.einsum('rnc,ncf->nrf', feature_rows, weight_groups)
        partials = lax.optimization_barrier(partials.astype(jnp.bfloat16)).astype(jnp.float32)
        projected = lax.optimization_barrier(jnp.sum(partials, axis=0)).reshape(token_count, KVH, 2, HD)
        key_heads = normalize_rows(projected[:, :, 0], k_gain).astype(jnp.bfloat16)
        value_heads = projected[:, :, 1].astype(jnp.bfloat16)
        query_here = normalize_rows(query_blocks[slot_id].astype(jnp.float32), q_gain) / math.sqrt(HD)
        query_here = lax.optimization_barrier(query_here.astype(jnp.bfloat16)).astype(jnp.float32)
        key_here = jnp.repeat(key_heads, group_size, axis=1).astype(jnp.float32)
        value_here = jnp.repeat(value_heads, group_size, axis=1).astype(jnp.float32)
        scores = jnp.einsum('tqd,rqd->qtr', query_here, key_here)
        valid_keys = jnp.arange(token_count, dtype=jnp.int32) < counts[sample] * PATCH
        exponent = jnp.where(valid_keys[None, None, :], jnp.exp(scores), 0.0)
        weights = (exponent / lax.optimization_barrier(jnp.sum(exponent, axis=-1, keepdims=True))).astype(jnp.bfloat16)
        weights = lax.optimization_barrier(weights).astype(jnp.float32)
        context = jnp.einsum('qtr,rqd->tqd', weights, value_here)
        return context.astype(jnp.bfloat16).reshape(TXT, QH * HD)
    attended = lax.map(attend_slot, jnp.arange(SAMPLES, dtype=jnp.int32))
    return attended.reshape(SAMPLES * TXT, QH * HD)
```

```python
import functools
import math

import jax
import jax.numpy as jnp
from jax import lax
from jax.experimental import pallas as pl
from jax.experimental.pallas import tpu as pltpu
from jax.sharding import PartitionSpec as P

KVH = 8
HD = 128
PATCH = 24
EPS = 1e-05
MESH = pl.DeviceIdType.MESH
MOST_VARIANTS = 16
VMEM_LIMIT = 60 * 1024 * 1024


def bit_orders(count):
    bits = [1 << b for b in range(count.bit_length() - 1)]
    return bits, bits[::-1]


def send_round(order, d):
    for r, bit in enumerate(order):
        if d & bit:
            return r
    return len(order)


def project_kernel(n, shift, x_hbm, w_hbm, gain_ref, moved_ref, *rest):
    stay_refs = rest[:-9]
    xv, wv, part, recv, ready, x_sem, w_sem, send_sem, recv_sem = rest[-9:]
    me = lax.axis_index("tensor")
    samples, tokens = xv.shape[0], xv.shape[1]
    half = tokens // 2
    width = wv.shape[2]
    orders = bit_orders(n)
    move_slot = 2 * samples * (n - 1)

    def flipped(d):
        result = me
        for bit in orders[0]:
            if d & bit:
                result = result + bit * (1 - 2 * ((me // bit) % 2))
        return result

    rounds = [[send_round(order, d) for d in range(n)] for order in orders]
    d_order = sorted(range(n), key=lambda d: (min(rounds[0][d], rounds[1][d]), -d))
    place_of = {d: i for i, d in enumerate(d_order)}
    later = sorted(
        [(rounds[s][d], -d, s) for d in range(1, n) for s in range(2) if rounds[s][d] > 0]
    )

    def x_copy(j):
        return pltpu.make_async_copy(x_hbm.at[j], xv.at[j], x_sem.at[j])

    def w_copy(i, first_column):
        columns = pl.ds(pl.multiple_of(first_column, 128), width)
        return pltpu.make_async_copy(w_hbm.at[:, columns], wv.at[i], w_sem.at[i])

    def remote(j, d, s):
        slot = (j * 2 + s) * (n - 1) + d - 1
        return pltpu.make_async_remote_copy(
            src_ref=part.at[j, place_of[d], pl.ds(s * half, half)],
            dst_ref=recv.at[j, s, d - 1],
            send_sem=send_sem.at[slot],
            recv_sem=recv_sem.at[slot],
            device_id={"tensor": flipped(orders[s][rounds[s][d]])},
            device_id_type=MESH,
        )

    def move(s):
        rows = pl.ds(s * half, half)
        if shift == 0:
            return pltpu.make_async_copy(
                ready.at[rows], moved_ref.at[rows], send_sem.at[move_slot + s]
            )
        return pltpu.make_async_remote_copy(
            src_ref=ready.at[rows],
            dst_ref=moved_ref.at[rows],
            send_sem=send_sem.at[move_slot + s],
            recv_sem=recv_sem.at[move_slot + s],
            device_id={"dp": lax.rem(place + shift, shard_count)},
            device_id_type=MESH,
        )

    shard_count = lax.axis_size("dp")
    place = lax.axis_index("dp")
    barrier = pltpu.get_barrier_semaphore()
    greeted = 0
    for bit in orders[0]:
        pl.semaphore_signal(barrier, inc=1, device_id={"tensor": flipped(bit)}, device_id_type=MESH)
        greeted += 1
    if shift:
        for by in (shift, shard_count - shift):
            other = lax.rem(place + by, shard_count)
            pl.semaphore_signal(barrier, inc=1, device_id={"dp": other}, device_id_type=MESH)
            greeted += 1
    x_copy(0).start()
    for i, d in enumerate(d_order):
        w_copy(i, flipped(d) * width).start()
    for j in range(1, samples):
        x_copy(j).start()

    def total(j, d, s):
        result = part[j, place_of[d], s * half : (s + 1) * half].astype(jnp.float32)
        for bit in orders[s][: rounds[s][d]]:
            remote(j, d | bit, s).wait_recv()
            result = result + recv[j, s, (d | bit) - 1].astype(jnp.float32)
        return result

    def send_later(j):
        for _, negative, s in later:
            d = -negative
            part[j, place_of[d], s * half : (s + 1) * half] = total(j, d, s).astype(jnp.bfloat16)
            remote(j, d, s).start()

    def finish(j):
        gain = gain_ref[...]
        target = ready if j == 0 else stay_refs[j - 1]
        for s in range(2):
            summed = total(j, 0, s)
            rows = slice(s * half, (s + 1) * half)
            for c in range(0, width, HD):
                block = summed[:, c : c + HD]
                if c // HD % 2 == 0:
                    scale = lax.rsqrt(jnp.mean(block * block, axis=-1, keepdims=True) + EPS)
                    block = block * scale * gain
                target[rows, c : c + HD] = block.astype(jnp.bfloat16)
            if j == 0:
                move(s).start()

    @pl.loop(0, samples * n)
    def _(step):
        j = step // n
        i = step % n

        @pl.when(i == 0)
        def _():
            x_copy(j).wait()

        @pl.when(j == 0)
        def _():
            w_copy(i, 0).wait()

        part[j, i] = jnp.dot(xv[j], wv[i], preferred_element_type=jnp.float32).astype(
            jnp.bfloat16
        )

        @pl.when(step == 0)
        def _():
            pl.semaphore_wait(barrier, greeted)

        if samples > 1:

            @pl.when((i == 0) & (j > 0))
            def _():
                send_later(j - 1)

        for k, d in enumerate(d_order):
            streams = [s for s in range(2) if rounds[s][d] == 0]
            if streams:

                @pl.when(i == k)
                def _():
                    for s in streams:
                        remote(j, d, s).start()

    for j in range(samples - 1):
        finish(j)
    send_later(samples - 1)
    finish(samples - 1)
    for j in range(samples):
        for d in range(1, n):
            for s in range(2):
                remote(j, d, s).wait_send()
    for s in range(2):
        move(s).wait()


def project(features, weight, k_gain, n, shift, collective_id):
    samples, tokens, channels = features.shape
    width = weight.shape[1] // n
    count = 2 * samples * (n - 1) + 2
    block = jax.ShapeDtypeStruct((tokens, width), jnp.bfloat16)
    return pl.pallas_call(
        functools.partial(project_kernel, n, shift),
        out_shape=[block] * samples,
        in_specs=[
            pl.BlockSpec(memory_space=pl.ANY),
            pl.BlockSpec(memory_space=pl.ANY),
            pl.BlockSpec(memory_space=pltpu.VMEM),
        ],
        out_specs=[pl.BlockSpec(memory_space=pl.ANY)]
        + [pl.BlockSpec(memory_space=pltpu.VMEM)] * (samples - 1),
        scratch_shapes=[
            pltpu.VMEM((samples, tokens, channels), jnp.bfloat16),
            pltpu.VMEM((n, channels, width), jnp.bfloat16),
            pltpu.VMEM((samples, n, tokens, width), jnp.bfloat16),
            pltpu.VMEM((samples, 2, n - 1, tokens // 2, width), jnp.bfloat16),
            pltpu.VMEM((tokens, width), jnp.bfloat16),
            pltpu.SemaphoreType.DMA((samples,)),
            pltpu.SemaphoreType.DMA((n,)),
            pltpu.SemaphoreType.DMA((count,)),
            pltpu.SemaphoreType.DMA((count,)),
        ],
        compiler_params=pltpu.CompilerParams(
            collective_id=collective_id, has_side_effects=True, vmem_limit_bytes=VMEM_LIMIT
        ),
        name="project",
    )(features, weight, k_gain)


def shift_rank(shard_count):
    def hops(c):
        return sum(abs((e + c) % shard_count // 2 - e // 2) for e in range(shard_count))

    return [hops(c) * shard_count - c for c in range(shard_count)]


def shift_pairs(shard_count):
    rank = shift_rank(shard_count)
    pairs = [(a, b) for a in range(shard_count) for b in range(a + 1, shard_count)]
    return [pair if rank[pair[0]] > rank[pair[1]] else pair[::-1] for pair in pairs]


def gather_kernel(
    shifts, owner_ref, x_hbm, w_hbm, gain_ref, kv_ref,
    xa, xb, xs, wv, part, recv0, mid, recv1, ready,
    x_sem, w_sem, send_sem, recv_sem,
):
    me = lax.axis_index("tensor")
    place = lax.axis_index("dp")
    shard_count = lax.axis_size("dp")
    blocks = part.shape[0]
    half_blocks = blocks // 2
    xv = (xa, xb)
    pieces = wv.shape[0]
    rows = part.shape[4]
    samples = 2

    def flipped(bit):
        return me + bit * (1 - 2 * ((me // bit) % 2))

    def slab(d):
        result = me
        if d & 1:
            result = result + 1 - 2 * (result % 2)
        if d & 2:
            result = result + 2 * (1 - 2 * ((me // 2) % 2))
        return result

    barrier = pltpu.get_barrier_semaphore()
    greeted = 0
    for bit in (1, 2):
        pl.semaphore_signal(barrier, inc=1, device_id={"tensor": flipped(bit)}, device_id_type=MESH)
        greeted += 1
    for c in shifts:
        if c:
            for by in (c, shard_count - c):
                other = lax.rem(place + by, shard_count)
                pl.semaphore_signal(barrier, inc=1, device_id={"dp": other}, device_id_type=MESH)
                greeted += 1

    block_rows = xs.shape[0]

    def x_copy(t, j):
        return pltpu.make_async_copy(
            x_hbm.at[j, pl.ds(t * block_rows, block_rows)], xv[t].at[j], x_sem.at[t * samples + j]
        )

    def w_copy(q, first):
        columns = pl.ds(pl.multiple_of(first, 128), wv.shape[2])
        return pltpu.make_async_copy(w_hbm.at[:, columns], wv.at[q], w_sem.at[q])

    for j in range(samples):
        x_copy(0, j).start()
    for i, d in enumerate((1, 3, 2, 0)):
        for half in range(2):
            w_copy(2 * i + half, slab(d) * 2 * wv.shape[2] + half * wv.shape[2]).start()
    for t in range(1, half_blocks):
        for j in range(samples):
            x_copy(t, j).start()

    swapped = (owner_ref[0] != samples * shifts[0]).astype(jnp.int32)

    def first_round(b, u, s):
        k = (b * 2 + u) * 2 + s
        return pltpu.make_async_remote_copy(
            src_ref=part.at[b, pl.ds(2 * s, 4), u, s],
            dst_ref=recv0.at[b, u, s],
            send_sem=send_sem.at[0, k],
            recv_sem=recv_sem.at[0, k],
            device_id={"tensor": flipped(1 + s)},
            device_id_type=MESH,
        )

    def second_round(b, u, s):
        k = (b * 2 + u) * 2 + s
        return pltpu.make_async_remote_copy(
            src_ref=mid.at[b, u, s],
            dst_ref=recv1.at[b, u, s],
            send_sem=send_sem.at[1, k],
            recv_sem=recv_sem.at[1, k],
            device_id={"tensor": flipped(2 - s)},
            device_id_type=MESH,
        )

    def move(c, b, u, s):
        k = (b * 2 + u) * 2 + s
        return pltpu.make_async_remote_copy(
            src_ref=ready.at[k],
            dst_ref=kv_ref.at[k],
            send_sem=send_sem.at[2, k],
            recv_sem=recv_sem.at[2, k],
            device_id={"dp": lax.rem(place + c, shard_count)},
            device_id_type=MESH,
        )

    phase_blocks = blocks // samples

    @pl.loop(0, blocks + 2)
    def _(step):
        @pl.when(step < blocks)
        def _():
            b = step
            phase = b // half_blocks
            sample = swapped + phase * (1 - 2 * swapped)
            for t in range(half_blocks):

                @pl.when(b == t)
                def _():
                    for j in range(samples):
                        x_copy(t, j).wait()

                @pl.when(b % half_blocks == t)
                def _():
                    xs[...] = xv[t][sample]

            @pl.loop(0, pieces)
            def _(q):
                @pl.when(b == 0)
                def _():
                    w_copy(q, 0).wait()

                result = jnp.dot(xs[...], wv[q], preferred_element_type=jnp.float32)
                result = result.astype(jnp.bfloat16)
                for u in range(2):
                    for s in range(2):
                        r = (u * 2 + s) * rows
                        part[b, q, u, s] = result[r : r + rows]

                @pl.when((b == 0) & (q == 0))
                def _():
                    pl.semaphore_wait(barrier, greeted)

                for s in range(2):

                    @pl.when(q == 3 + 2 * s)
                    def _():
                        for u in range(2):
                            first_round(b, u, s).start()

        @pl.when((step >= 1) & (step <= blocks))
        def _():
            b = step - 1

            @pl.loop(0, 4)
            def _(k):
                u = k // 2
                s = k % 2
                first_round(b, u, s).wait_recv()
                for half in range(2):
                    mine = part[b, 4 * (1 - s) + half, u, s].astype(jnp.float32)
                    other = recv0[b, u, s, 2 * (1 - s) + half].astype(jnp.float32)
                    mid[b, u, s, half] = (mine + other).astype(jnp.bfloat16)
                second_round(b, u, s).start()

        @pl.when(step >= 2)
        def _():
            b = step - 2
            gain = gain_ref[...]

            @pl.loop(0, 4)
            def _(k):
                u = k // 2
                s = k % 2
                at = b * 4 + k
                second_round(b, u, s).wait_recv()
                for half in range(2):
                    block = part[b, 6 + half, u, s].astype(jnp.float32)
                    block = block + recv0[b, u, s, 2 * s + half].astype(jnp.float32)
                    block = block + recv1[b, u, s, half].astype(jnp.float32)
                    key = block[:, :HD]
                    scale = lax.rsqrt(jnp.mean(key * key, axis=-1, keepdims=True) + EPS)
                    ready[at, half, :, :HD] = (key * scale * gain).astype(jnp.bfloat16)
                    ready[at, half, :, HD:] = block[:, HD:].astype(jnp.bfloat16)
                for ph, c in enumerate(shifts):

                    @pl.when(b // phase_blocks == ph)
                    def _():
                        if c == 0:
                            kv_ref[at] = ready[at]
                        else:
                            move(c, b, u, s).start()

    @pl.loop(0, blocks * 4)
    def _(k):
        b = k // 4
        u = (k // 2) % 2
        s = k % 2
        first_round(b, u, s).wait_send()
        second_round(b, u, s).wait_send()
        for ph, c in enumerate(shifts):
            if c:

                @pl.when(b // phase_blocks == ph)
                def _():
                    move(c, b, u, s).wait()


def gather(owner, features, weight, k_gain, shifts, collective_id):
    samples, tokens, channels = features.shape
    width = weight.shape[1] // lax.axis_size("tensor")
    rows = 48
    block_rows = 4 * rows
    per_sample = tokens // block_rows
    blocks = samples * per_sample
    piece = width // 2
    count = blocks * 4
    bf16 = jnp.bfloat16
    any_space = pl.BlockSpec(memory_space=pl.ANY)
    return pl.pallas_call(
        functools.partial(gather_kernel, shifts),
        out_shape=jax.ShapeDtypeStruct((count, 2, rows, piece), bf16),
        in_specs=[
            pl.BlockSpec(memory_space=pltpu.SMEM),
            any_space,
            any_space,
            pl.BlockSpec(memory_space=pltpu.VMEM),
        ],
        out_specs=pl.BlockSpec(memory_space=pltpu.VMEM),
        scratch_shapes=[
            pltpu.VMEM((samples, block_rows, channels), bf16),
            pltpu.VMEM((samples, block_rows, channels), bf16),
            pltpu.VMEM((block_rows, channels), bf16),
            pltpu.VMEM((8, channels, piece), bf16),
            pltpu.VMEM((blocks, 8, 2, 2, rows, piece), bf16),
            pltpu.VMEM((blocks, 2, 2, 4, rows, piece), bf16),
            pltpu.VMEM((blocks, 2, 2, 2, rows, piece), bf16),
            pltpu.VMEM((blocks, 2, 2, 2, rows, piece), bf16),
            pltpu.VMEM((count, 2, rows, piece), bf16),
            pltpu.SemaphoreType.DMA((blocks,)),
            pltpu.SemaphoreType.DMA((8,)),
            pltpu.SemaphoreType.DMA((3, count)),
            pltpu.SemaphoreType.DMA((3, count)),
        ],
        compiler_params=pltpu.CompilerParams(
            collective_id=collective_id, has_side_effects=True, vmem_limit_bytes=VMEM_LIMIT
        ),
        name="gather",
    )(owner, features, weight, k_gain)


def attend_all_kernel(samples, count_ref, owner_ref, q_ref, gain_ref, kv_ref, out_ref):
    shard_count = lax.axis_size("dp")
    j = pl.program_id(0)
    h = pl.program_id(1)
    slots, _, rows, piece = kv_ref.shape
    per_sample = slots // samples
    tokens = per_sample * rows
    shifts = [owner_ref[i] // samples for i in range(samples)]
    ranks = [
        sum(jnp.where(c == i, r, 0) for i, r in enumerate(shift_rank(shard_count))) for c in shifts
    ]
    swapped = (ranks[0] < ranks[1]).astype(jnp.int32)
    phase = swapped + j * (1 - 2 * swapped)
    shift = jnp.where(j == 0, shifts[0], shifts[1])
    source = lax.rem(lax.axis_index("dp") - shift + shard_count, shard_count)
    count = count_ref[source * samples + j]
    keys = kv_ref[pl.ds(phase * per_sample, per_sample), h, :, :HD].reshape(tokens, HD)
    values = kv_ref[pl.ds(phase * per_sample, per_sample), h, :, HD:].reshape(tokens, HD)
    valid = lax.broadcasted_iota(jnp.int32, (tokens, HD), 0) < count * PATCH
    values = jnp.concatenate(
        [
            jnp.where(valid, values.astype(jnp.float32), 0.0).astype(jnp.bfloat16),
            jnp.where(valid, 1.0, 0.0).astype(jnp.bfloat16),
        ],
        axis=1,
    )
    gain = gain_ref[...] * (1.0 / math.sqrt(HD))
    for head in range(q_ref.shape[1] // HD):
        columns = slice(head * HD, (head + 1) * HD)
        query = q_ref[:, columns].astype(jnp.float32)
        scale = lax.rsqrt(jnp.mean(query * query, axis=-1, keepdims=True) + EPS)
        query = (query * scale * gain).astype(jnp.bfloat16)
        scores = lax.dot_general(
            query, keys, (((1,), (1,)), ((), ())), preferred_element_type=jnp.float32
        )
        weights = jnp.exp(scores).astype(jnp.bfloat16)
        both = jnp.dot(weights, values, preferred_element_type=jnp.float32)
        out_ref[:, columns] = (both[:, :HD] / both[:, HD:]).astype(jnp.bfloat16)


def attend_all(counts, owner, queries, q_gain, kv, samples):
    kv_heads = kv.shape[1]
    text_len = queries.shape[0] // samples
    group = queries.shape[1] // kv_heads
    smem = pl.BlockSpec(memory_space=pltpu.SMEM)
    return pl.pallas_call(
        functools.partial(attend_all_kernel, samples),
        out_shape=jax.ShapeDtypeStruct(queries.shape, jnp.bfloat16),
        grid=(samples, kv_heads),
        in_specs=[
            smem,
            smem,
            pl.BlockSpec((text_len, group), lambda j, h: (j, h)),
            pl.BlockSpec((1, HD), lambda j, h: (0, 0)),
            pl.BlockSpec(memory_space=pltpu.VMEM),
        ],
        out_specs=pl.BlockSpec((text_len, group), lambda j, h: (j, h)),
        name="attend_all",
    )(counts, owner, queries, q_gain.reshape(1, HD), kv)


def attend_kernel(sample, samples, count_ref, owner_ref, q_ref, gain_ref, kv_ref, *rest):
    out_ref = rest[-1]
    shard_count = lax.axis_size("dp")
    tokens = kv_ref.shape[0]
    source = lax.axis_index("dp") - owner_ref[sample] // samples + shard_count
    count = count_ref[lax.rem(source, shard_count) * samples + sample]
    keys = kv_ref[:, :HD]
    values = jnp.concatenate([kv_ref[:, HD:], jnp.ones((tokens, HD), jnp.bfloat16)], axis=1)
    valid = lax.broadcasted_iota(jnp.int32, (1, tokens), 1) < count * PATCH
    gain = gain_ref[...] * (1.0 / math.sqrt(HD))
    for head in range(q_ref.shape[1] // HD):
        columns = slice(head * HD, (head + 1) * HD)
        query = q_ref[:, columns].astype(jnp.float32)
        scale = lax.rsqrt(jnp.mean(query * query, axis=-1, keepdims=True) + EPS)
        query = (query * scale * gain).astype(jnp.bfloat16)
        scores = lax.dot_general(
            query, keys, (((1,), (1,)), ((), ())), preferred_element_type=jnp.float32
        )
        weights = jnp.where(valid, jnp.exp(scores), 0.0).astype(jnp.bfloat16)
        both = jnp.dot(weights, values, preferred_element_type=jnp.float32)
        out_ref[:, columns] = (both[:, :HD] / both[:, HD:]).astype(jnp.bfloat16)


def attend(sample, samples, counts, owner, queries, q_gain, kv, out):
    tokens, width = kv.shape
    kv_heads = width // (2 * HD)
    text_len = queries.shape[0] // samples
    group = queries.shape[1] // kv_heads
    smem = pl.BlockSpec(memory_space=pltpu.SMEM)
    operands = [counts, owner, queries, q_gain.reshape(1, HD), kv]
    specs = [
        smem,
        smem,
        pl.BlockSpec((text_len, group), lambda h: (sample, h)),
        pl.BlockSpec((1, HD), lambda h: (0, 0)),
        pl.BlockSpec((tokens, 2 * HD), lambda h: (0, h)),
    ]
    aliases = {}
    if out is not None:
        aliases = {len(operands): 0}
        operands.append(out)
        specs.append(pl.BlockSpec(memory_space=pl.ANY))
    products = 2 * text_len * queries.shape[1] * tokens * 2
    return pl.pallas_call(
        functools.partial(attend_kernel, sample, samples),
        out_shape=jax.ShapeDtypeStruct(queries.shape, jnp.bfloat16),
        grid=(kv_heads,),
        in_specs=specs,
        out_specs=pl.BlockSpec((text_len, group), lambda h: (sample, h)),
        input_output_aliases=aliases,
        cost_estimate=pl.CostEstimate(
            flops=products, bytes_accessed=4 * text_len * queries.shape[1], transcendentals=0
        ),
        name="attend",
    )(*operands)


def shift_by(value, count):
    if count == 0:
        return value
    length = lax.axis_size("dp")
    return lax.ppermute(value, "dp", [(i, (i + count) % length) for i in range(length)])


def shards(queries, features, kv_weight, q_gain, k_gain, counts, owner):
    samples_here, token_count, channels = features.shape
    shard_count = lax.axis_size("dp")
    tensor_count = lax.axis_size("tensor")
    local_width = kv_weight.shape[1] // tensor_count
    repeats = max(1, 2 * HD // local_width)
    if repeats > 1:
        weight_used = jnp.repeat(kv_weight.reshape(channels, KVH, 2 * HD), repeats, axis=1)
        weight_used = weight_used.reshape(channels, KVH * repeats * 2 * HD)
    else:
        weight_used = kv_weight
    gain = k_gain.reshape(1, HD)
    if shard_count <= MOST_VARIANTS and tensor_count == 4 and samples_here == 2:
        first, second = owner[0] // samples_here, owner[1] // samples_here
        low, high = jnp.minimum(first, second), jnp.maximum(first, second)
        index = low * (2 * shard_count - 1 - low) // 2 + high - low - 1
        branches = [
            functools.partial(gather, shifts=pair, collective_id=i)
            for i, pair in enumerate(shift_pairs(shard_count))
        ]
        kv = lax.switch(index, branches, owner, features, kv_weight, gain)
        return attend_all(counts, owner, queries, q_gain, kv, samples_here)
    shifts = owner // samples_here

    def first_stage(c):
        return lambda: project(features, weight_used, gain, tensor_count, c, c)

    def attend_one(j, kv, out):
        return attend(j, samples_here, counts, owner, queries, q_gain, kv, out)

    def next_stage(j, c):
        return lambda value, kv, out: (shift_by(value, c), attend_one(j - 1, kv, out))

    def shift_switch(j, value):
        moves = [functools.partial(shift_by, count=c) for c in range(shard_count)]
        return lax.switch(shifts[j], moves, value)

    out = None
    if shard_count > MOST_VARIANTS:
        held = first_stage(0)()
        for j in range(samples_here):
            out = attend_one(j, shift_switch(j, held[j]), out)
        return out
    held = lax.switch(shifts[0], [first_stage(c) for c in range(shard_count)])
    moved = held[0]
    for j in range(1, samples_here):
        stages = [next_stage(j, c) for c in range(shard_count)]
        moved, out = lax.switch(shifts[j], stages, held[j], moved, out)
    return attend_one(samples_here - 1, moved, out)


def solution(mesh):
    placed = (P("dp", "tensor"), P("dp", None, "tensor"), P("tensor", None), P(), P(), P(), P())
    return jax.shard_map(
        shards, mesh=mesh, in_specs=placed, out_specs=P("dp", "tensor"), check_vma=False
    )
```

```python
import functools
import math

import jax
import jax.numpy as jnp
from jax import lax
from jax.experimental import pallas as pl
from jax.experimental.pallas import tpu as pltpu
from jax.sharding import PartitionSpec as P

KVH = 8
HD = 128
PATCH = 24
EPS = 1e-05
MESH = pl.DeviceIdType.MESH
MOST_VARIANTS = 16
FORWARD_LAG = 2
FINISH_LAG = 4
GATHER_VMEM = 58 * 1024 * 1024
VMEM_LIMIT = 60 * 1024 * 1024


def bit_orders(count):
    bits = [1 << b for b in range(count.bit_length() - 1)]
    return bits, bits[::-1]


def send_round(order, d):
    for r, bit in enumerate(order):
        if d & bit:
            return r
    return len(order)


def project_kernel(n, shift, x_hbm, w_hbm, gain_ref, moved_ref, *rest):
    stay_refs = rest[:-9]
    xv, wv, part, recv, ready, x_sem, w_sem, send_sem, recv_sem = rest[-9:]
    me = lax.axis_index("tensor")
    samples, tokens = xv.shape[0], xv.shape[1]
    half = tokens // 2
    width = wv.shape[2]
    orders = bit_orders(n)
    move_slot = 2 * samples * (n - 1)

    def flipped(d):
        result = me
        for bit in orders[0]:
            if d & bit:
                result = result + bit * (1 - 2 * ((me // bit) % 2))
        return result

    rounds = [[send_round(order, d) for d in range(n)] for order in orders]
    d_order = sorted(range(n), key=lambda d: (min(rounds[0][d], rounds[1][d]), -d))
    place_of = {d: i for i, d in enumerate(d_order)}
    later = sorted(
        [(rounds[s][d], -d, s) for d in range(1, n) for s in range(2) if rounds[s][d] > 0]
    )

    def x_copy(j):
        return pltpu.make_async_copy(x_hbm.at[j], xv.at[j], x_sem.at[j])

    def w_copy(i, first_column):
        columns = pl.ds(pl.multiple_of(first_column, 128), width)
        return pltpu.make_async_copy(w_hbm.at[:, columns], wv.at[i], w_sem.at[i])

    def remote(j, d, s):
        slot = (j * 2 + s) * (n - 1) + d - 1
        return pltpu.make_async_remote_copy(
            src_ref=part.at[j, place_of[d], pl.ds(s * half, half)],
            dst_ref=recv.at[j, s, d - 1],
            send_sem=send_sem.at[slot],
            recv_sem=recv_sem.at[slot],
            device_id={"tensor": flipped(orders[s][rounds[s][d]])},
            device_id_type=MESH,
        )

    def move(s):
        rows = pl.ds(s * half, half)
        if shift == 0:
            return pltpu.make_async_copy(
                ready.at[rows], moved_ref.at[rows], send_sem.at[move_slot + s]
            )
        return pltpu.make_async_remote_copy(
            src_ref=ready.at[rows],
            dst_ref=moved_ref.at[rows],
            send_sem=send_sem.at[move_slot + s],
            recv_sem=recv_sem.at[move_slot + s],
            device_id={"dp": lax.rem(place + shift, shard_count)},
            device_id_type=MESH,
        )

    shard_count = lax.axis_size("dp")
    place = lax.axis_index("dp")
    barrier = pltpu.get_barrier_semaphore()
    greeted = 0
    for bit in orders[0]:
        pl.semaphore_signal(barrier, inc=1, device_id={"tensor": flipped(bit)}, device_id_type=MESH)
        greeted += 1
    if shift:
        for by in (shift, shard_count - shift):
            other = lax.rem(place + by, shard_count)
            pl.semaphore_signal(barrier, inc=1, device_id={"dp": other}, device_id_type=MESH)
            greeted += 1
    x_copy(0).start()
    for i, d in enumerate(d_order):
        w_copy(i, flipped(d) * width).start()
    for j in range(1, samples):
        x_copy(j).start()

    def total(j, d, s):
        result = part[j, place_of[d], s * half : (s + 1) * half].astype(jnp.float32)
        for bit in orders[s][: rounds[s][d]]:
            remote(j, d | bit, s).wait_recv()
            result = result + recv[j, s, (d | bit) - 1].astype(jnp.float32)
        return result

    def send_later(j):
        for _, negative, s in later:
            d = -negative
            part[j, place_of[d], s * half : (s + 1) * half] = total(j, d, s).astype(jnp.bfloat16)
            remote(j, d, s).start()

    def finish(j):
        gain = gain_ref[...]
        target = ready if j == 0 else stay_refs[j - 1]
        for s in range(2):
            summed = total(j, 0, s)
            rows = slice(s * half, (s + 1) * half)
            for c in range(0, width, HD):
                block = summed[:, c : c + HD]
                if c // HD % 2 == 0:
                    scale = lax.rsqrt(jnp.mean(block * block, axis=-1, keepdims=True) + EPS)
                    block = block * scale * gain
                target[rows, c : c + HD] = block.astype(jnp.bfloat16)
            if j == 0:
                move(s).start()

    @pl.loop(0, samples * n)
    def _(step):
        j = step // n
        i = step % n

        @pl.when(i == 0)
        def _():
            x_copy(j).wait()

        @pl.when(j == 0)
        def _():
            w_copy(i, 0).wait()

        part[j, i] = jnp.dot(xv[j], wv[i], preferred_element_type=jnp.float32).astype(
            jnp.bfloat16
        )

        @pl.when(step == 0)
        def _():
            pl.semaphore_wait(barrier, greeted)

        if samples > 1:

            @pl.when((i == 0) & (j > 0))
            def _():
                send_later(j - 1)

        for k, d in enumerate(d_order):
            streams = [s for s in range(2) if rounds[s][d] == 0]
            if streams:

                @pl.when(i == k)
                def _():
                    for s in streams:
                        remote(j, d, s).start()

    for j in range(samples - 1):
        finish(j)
    send_later(samples - 1)
    finish(samples - 1)
    for j in range(samples):
        for d in range(1, n):
            for s in range(2):
                remote(j, d, s).wait_send()
    for s in range(2):
        move(s).wait()


def project(features, weight, k_gain, n, shift, collective_id):
    samples, tokens, channels = features.shape
    width = weight.shape[1] // n
    count = 2 * samples * (n - 1) + 2
    block = jax.ShapeDtypeStruct((tokens, width), jnp.bfloat16)
    return pl.pallas_call(
        functools.partial(project_kernel, n, shift),
        out_shape=[block] * samples,
        in_specs=[
            pl.BlockSpec(memory_space=pl.ANY),
            pl.BlockSpec(memory_space=pl.ANY),
            pl.BlockSpec(memory_space=pltpu.VMEM),
        ],
        out_specs=[pl.BlockSpec(memory_space=pl.ANY)]
        + [pl.BlockSpec(memory_space=pltpu.VMEM)] * (samples - 1),
        scratch_shapes=[
            pltpu.VMEM((samples, tokens, channels), jnp.bfloat16),
            pltpu.VMEM((n, channels, width), jnp.bfloat16),
            pltpu.VMEM((samples, n, tokens, width), jnp.bfloat16),
            pltpu.VMEM((samples, 2, n - 1, tokens // 2, width), jnp.bfloat16),
            pltpu.VMEM((tokens, width), jnp.bfloat16),
            pltpu.SemaphoreType.DMA((samples,)),
            pltpu.SemaphoreType.DMA((n,)),
            pltpu.SemaphoreType.DMA((count,)),
            pltpu.SemaphoreType.DMA((count,)),
        ],
        compiler_params=pltpu.CompilerParams(
            collective_id=collective_id, has_side_effects=True, vmem_limit_bytes=VMEM_LIMIT
        ),
        name="project",
    )(features, weight, k_gain)


def shift_rank(shard_count):
    def hops(c):
        return sum(abs((e + c) % shard_count // 2 - e // 2) for e in range(shard_count))

    return [hops(c) * shard_count - c for c in range(shard_count)]


def shift_pairs(shard_count):
    rank = shift_rank(shard_count)
    pairs = [(a, b) for a in range(shard_count) for b in range(a + 1, shard_count)]
    return [pair if rank[pair[0]] > rank[pair[1]] else pair[::-1] for pair in pairs]


def gather_kernel(
    shifts, owner_ref, x_hbm, w_hbm, gain_ref, kv_ref,
    xa, xb, xs, wv, part, recv0, mid, recv1, ready,
    x_sem, w_sem, send_sem, recv_sem,
):
    me = lax.axis_index("tensor")
    place = lax.axis_index("dp")
    shard_count = lax.axis_size("dp")
    blocks = part.shape[0]
    half_blocks = blocks // 2
    xv = (xa, xb)
    pieces = wv.shape[0]
    rows = part.shape[4]
    samples = 2

    def flipped(bit):
        return me + bit * (1 - 2 * ((me // bit) % 2))

    def slab(d):
        result = me
        if d & 1:
            result = result + 1 - 2 * (result % 2)
        if d & 2:
            result = result + 2 * (1 - 2 * ((me // 2) % 2))
        return result

    barrier = pltpu.get_barrier_semaphore()
    greeted = 0
    for bit in (1, 2):
        pl.semaphore_signal(barrier, inc=1, device_id={"tensor": flipped(bit)}, device_id_type=MESH)
        greeted += 1
    for c in shifts:
        if c:
            for by in (c, shard_count - c):
                other = lax.rem(place + by, shard_count)
                pl.semaphore_signal(barrier, inc=1, device_id={"dp": other}, device_id_type=MESH)
                greeted += 1

    block_rows = xs.shape[0]

    def x_copy(t, j):
        return pltpu.make_async_copy(
            x_hbm.at[j, pl.ds(t * block_rows, block_rows)], xv[t].at[j], x_sem.at[t * samples + j]
        )

    def w_copy(q, first):
        columns = pl.ds(pl.multiple_of(first, 128), wv.shape[2])
        return pltpu.make_async_copy(w_hbm.at[:, columns], wv.at[q], w_sem.at[q])

    for j in range(samples):
        x_copy(0, j).start()
    for i, d in enumerate((1, 3, 2, 0)):
        for half in range(2):
            w_copy(2 * i + half, slab(d) * 2 * wv.shape[2] + half * wv.shape[2]).start()
    for t in range(1, half_blocks):
        for j in range(samples):
            x_copy(t, j).start()

    swapped = (owner_ref[0] != samples * shifts[0]).astype(jnp.int32)

    def first_round(b, u, s):
        k = (b * 2 + u) * 2 + s
        return pltpu.make_async_remote_copy(
            src_ref=part.at[b, pl.ds(2 * s, 4), u, s],
            dst_ref=recv0.at[b, u, s],
            send_sem=send_sem.at[0, k],
            recv_sem=recv_sem.at[0, k],
            device_id={"tensor": flipped(1 + s)},
            device_id_type=MESH,
        )

    def second_round(b, u, s):
        k = (b * 2 + u) * 2 + s
        return pltpu.make_async_remote_copy(
            src_ref=mid.at[b, u, s],
            dst_ref=recv1.at[b, u, s],
            send_sem=send_sem.at[1, k],
            recv_sem=recv_sem.at[1, k],
            device_id={"tensor": flipped(2 - s)},
            device_id_type=MESH,
        )

    def move(c, b, u, s):
        k = (b * 2 + u) * 2 + s
        return pltpu.make_async_remote_copy(
            src_ref=ready.at[k],
            dst_ref=kv_ref.at[k],
            send_sem=send_sem.at[2, k],
            recv_sem=recv_sem.at[2, k],
            device_id={"dp": lax.rem(place + c, shard_count)},
            device_id_type=MESH,
        )

    def compute(b):
        phase = b // half_blocks
        sample = swapped + phase * (1 - 2 * swapped)
        for t in range(half_blocks):

            @pl.when(b == t)
            def _():
                for j in range(samples):
                    x_copy(t, j).wait()

            @pl.when(b % half_blocks == t)
            def _():
                xs[...] = xv[t][sample]

        @pl.loop(0, pieces)
        def _(q):
            @pl.when(b == 0)
            def _():
                w_copy(q, 0).wait()

            result = jnp.dot(xs[...], wv[q], preferred_element_type=jnp.float32)
            result = result.astype(jnp.bfloat16)
            for u in range(2):
                for s in range(2):
                    r = (u * 2 + s) * rows
                    part[b, q, u, s] = result[r : r + rows]

            for s in range(2):

                @pl.when((b == 0) & (q == 3 + 2 * s))
                def _():
                    first_round(b, 0, s).start()

    def forward(b, u):
        @pl.loop(0, 2)
        def _(s):
            first_round(b, u, s).wait_recv()
            for half in range(2):
                mine = part[b, 4 * (1 - s) + half, u, s].astype(jnp.float32)
                other = recv0[b, u, s, 2 * (1 - s) + half].astype(jnp.float32)
                mid[b, u, s, half] = (mine + other).astype(jnp.bfloat16)
            second_round(b, u, s).start()

    def finish(b, u):
        gain = gain_ref[...]

        @pl.loop(0, 2)
        def _(s):
            at = b * 4 + u * 2 + s
            second_round(b, u, s).wait_recv()
            for half in range(2):
                block = part[b, 6 + half, u, s].astype(jnp.float32)
                block = block + recv0[b, u, s, 2 * s + half].astype(jnp.float32)
                block = block + recv1[b, u, s, half].astype(jnp.float32)
                key = block[:, :HD]
                scale = lax.rsqrt(jnp.mean(key * key, axis=-1, keepdims=True) + EPS)
                ready[at, half, :, :HD] = (key * scale * gain).astype(jnp.bfloat16)
                ready[at, half, :, HD:] = block[:, HD:].astype(jnp.bfloat16)
            for ph, c in enumerate(shifts):

                @pl.when(b // half_blocks == ph)
                def _():
                    if c == 0:
                        kv_ref[at] = ready[at]
                    else:
                        move(c, b, u, s).start()

    pl.semaphore_wait(barrier, greeted)

    @pl.loop(0, 2 * blocks + FINISH_LAG)
    def _(step):
        @pl.when((step % 2 == 0) & (step < 2 * blocks))
        def _():
            compute(step // 2)

        @pl.when((step >= 1) & (step < 2 * blocks))
        def _():
            for s in range(2):
                first_round(step // 2, step % 2, s).start()

        at = step - FORWARD_LAG

        @pl.when((at >= 0) & (at < 2 * blocks))
        def _():
            forward(at // 2, at % 2)

        last = step - FINISH_LAG

        @pl.when(last >= 0)
        def _():
            finish(last // 2, last % 2)

    @pl.loop(0, blocks * 4)
    def _(k):
        b = k // 4
        u = (k // 2) % 2
        s = k % 2
        first_round(b, u, s).wait_send()
        second_round(b, u, s).wait_send()
        for ph, c in enumerate(shifts):
            if c:

                @pl.when(b // half_blocks == ph)
                def _():
                    move(c, b, u, s).wait()


def gather(owner, features, weight, k_gain, shifts, collective_id):
    samples, tokens, channels = features.shape
    width = weight.shape[1] // lax.axis_size("tensor")
    rows = 48
    block_rows = 4 * rows
    per_sample = tokens // block_rows
    blocks = samples * per_sample
    piece = width // 2
    count = blocks * 4
    bf16 = jnp.bfloat16
    any_space = pl.BlockSpec(memory_space=pl.ANY)
    return pl.pallas_call(
        functools.partial(gather_kernel, shifts),
        out_shape=jax.ShapeDtypeStruct((count, 2, rows, piece), bf16),
        in_specs=[
            pl.BlockSpec(memory_space=pltpu.SMEM),
            any_space,
            any_space,
            pl.BlockSpec(memory_space=pltpu.VMEM),
        ],
        out_specs=pl.BlockSpec(memory_space=pltpu.VMEM),
        scratch_shapes=[
            pltpu.VMEM((samples, block_rows, channels), bf16),
            pltpu.VMEM((samples, block_rows, channels), bf16),
            pltpu.VMEM((block_rows, channels), bf16),
            pltpu.VMEM((8, channels, piece), bf16),
            pltpu.VMEM((blocks, 8, 2, 2, rows, piece), bf16),
            pltpu.VMEM((blocks, 2, 2, 4, rows, piece), bf16),
            pltpu.VMEM((blocks, 2, 2, 2, rows, piece), bf16),
            pltpu.VMEM((blocks, 2, 2, 2, rows, piece), bf16),
            pltpu.VMEM((count, 2, rows, piece), bf16),
            pltpu.SemaphoreType.DMA((blocks,)),
            pltpu.SemaphoreType.DMA((8,)),
            pltpu.SemaphoreType.DMA((3, count)),
            pltpu.SemaphoreType.DMA((3, count)),
        ],
        compiler_params=pltpu.CompilerParams(
            collective_id=collective_id, has_side_effects=True, vmem_limit_bytes=GATHER_VMEM
        ),
        name="gather",
    )(owner, features, weight, k_gain)


def attend_all_kernel(samples, count_ref, owner_ref, q_ref, gain_ref, kv_ref, out_ref):
    shard_count = lax.axis_size("dp")
    j = pl.program_id(0)
    h = pl.program_id(1)
    slots, _, rows, piece = kv_ref.shape
    per_sample = slots // samples
    tokens = per_sample * rows
    shifts = [owner_ref[i] // samples for i in range(samples)]
    ranks = [
        sum(jnp.where(c == i, r, 0) for i, r in enumerate(shift_rank(shard_count))) for c in shifts
    ]
    swapped = (ranks[0] < ranks[1]).astype(jnp.int32)
    phase = swapped + j * (1 - 2 * swapped)
    shift = jnp.where(j == 0, shifts[0], shifts[1])
    source = lax.rem(lax.axis_index("dp") - shift + shard_count, shard_count)
    count = count_ref[source * samples + j]
    keys = kv_ref[pl.ds(phase * per_sample, per_sample), h, :, :HD].reshape(tokens, HD)
    values = kv_ref[pl.ds(phase * per_sample, per_sample), h, :, HD:].reshape(tokens, HD)
    valid = lax.broadcasted_iota(jnp.int32, (tokens, HD), 0) < count * PATCH
    values = jnp.concatenate(
        [
            jnp.where(valid, values.astype(jnp.float32), 0.0).astype(jnp.bfloat16),
            jnp.where(valid, 1.0, 0.0).astype(jnp.bfloat16),
        ],
        axis=1,
    )
    gain = gain_ref[...] * (1.0 / math.sqrt(HD))
    for head in range(q_ref.shape[1] // HD):
        columns = slice(head * HD, (head + 1) * HD)
        query = q_ref[:, columns].astype(jnp.float32)
        scale = lax.rsqrt(jnp.mean(query * query, axis=-1, keepdims=True) + EPS)
        query = (query * scale * gain).astype(jnp.bfloat16)
        scores = lax.dot_general(
            query, keys, (((1,), (1,)), ((), ())), preferred_element_type=jnp.float32
        )
        weights = jnp.exp(scores).astype(jnp.bfloat16)
        both = jnp.dot(weights, values, preferred_element_type=jnp.float32)
        out_ref[:, columns] = (both[:, :HD] / both[:, HD:]).astype(jnp.bfloat16)


def attend_all(counts, owner, queries, q_gain, kv, samples):
    kv_heads = kv.shape[1]
    text_len = queries.shape[0] // samples
    group = queries.shape[1] // kv_heads
    smem = pl.BlockSpec(memory_space=pltpu.SMEM)
    return pl.pallas_call(
        functools.partial(attend_all_kernel, samples),
        out_shape=jax.ShapeDtypeStruct(queries.shape, jnp.bfloat16),
        grid=(samples, kv_heads),
        in_specs=[
            smem,
            smem,
            pl.BlockSpec((text_len, group), lambda j, h: (j, h)),
            pl.BlockSpec((1, HD), lambda j, h: (0, 0)),
            pl.BlockSpec(memory_space=pltpu.VMEM),
        ],
        out_specs=pl.BlockSpec((text_len, group), lambda j, h: (j, h)),
        name="attend_all",
    )(counts, owner, queries, q_gain.reshape(1, HD), kv)


def attend_kernel(sample, samples, count_ref, owner_ref, q_ref, gain_ref, kv_ref, *rest):
    out_ref = rest[-1]
    shard_count = lax.axis_size("dp")
    tokens = kv_ref.shape[0]
    source = lax.axis_index("dp") - owner_ref[sample] // samples + shard_count
    count = count_ref[lax.rem(source, shard_count) * samples + sample]
    keys = kv_ref[:, :HD]
    values = jnp.concatenate([kv_ref[:, HD:], jnp.ones((tokens, HD), jnp.bfloat16)], axis=1)
    valid = lax.broadcasted_iota(jnp.int32, (1, tokens), 1) < count * PATCH
    gain = gain_ref[...] * (1.0 / math.sqrt(HD))
    for head in range(q_ref.shape[1] // HD):
        columns = slice(head * HD, (head + 1) * HD)
        query = q_ref[:, columns].astype(jnp.float32)
        scale = lax.rsqrt(jnp.mean(query * query, axis=-1, keepdims=True) + EPS)
        query = (query * scale * gain).astype(jnp.bfloat16)
        scores = lax.dot_general(
            query, keys, (((1,), (1,)), ((), ())), preferred_element_type=jnp.float32
        )
        weights = jnp.where(valid, jnp.exp(scores), 0.0).astype(jnp.bfloat16)
        both = jnp.dot(weights, values, preferred_element_type=jnp.float32)
        out_ref[:, columns] = (both[:, :HD] / both[:, HD:]).astype(jnp.bfloat16)


def attend(sample, samples, counts, owner, queries, q_gain, kv, out):
    tokens, width = kv.shape
    kv_heads = width // (2 * HD)
    text_len = queries.shape[0] // samples
    group = queries.shape[1] // kv_heads
    smem = pl.BlockSpec(memory_space=pltpu.SMEM)
    operands = [counts, owner, queries, q_gain.reshape(1, HD), kv]
    specs = [
        smem,
        smem,
        pl.BlockSpec((text_len, group), lambda h: (sample, h)),
        pl.BlockSpec((1, HD), lambda h: (0, 0)),
        pl.BlockSpec((tokens, 2 * HD), lambda h: (0, h)),
    ]
    aliases = {}
    if out is not None:
        aliases = {len(operands): 0}
        operands.append(out)
        specs.append(pl.BlockSpec(memory_space=pl.ANY))
    products = 2 * text_len * queries.shape[1] * tokens * 2
    return pl.pallas_call(
        functools.partial(attend_kernel, sample, samples),
        out_shape=jax.ShapeDtypeStruct(queries.shape, jnp.bfloat16),
        grid=(kv_heads,),
        in_specs=specs,
        out_specs=pl.BlockSpec((text_len, group), lambda h: (sample, h)),
        input_output_aliases=aliases,
        cost_estimate=pl.CostEstimate(
            flops=products, bytes_accessed=4 * text_len * queries.shape[1], transcendentals=0
        ),
        name="attend",
    )(*operands)


def shift_by(value, count):
    if count == 0:
        return value
    length = lax.axis_size("dp")
    return lax.ppermute(value, "dp", [(i, (i + count) % length) for i in range(length)])


def shards(queries, features, kv_weight, q_gain, k_gain, counts, owner):
    samples_here, token_count, channels = features.shape
    shard_count = lax.axis_size("dp")
    tensor_count = lax.axis_size("tensor")
    local_width = kv_weight.shape[1] // tensor_count
    repeats = max(1, 2 * HD // local_width)
    if repeats > 1:
        weight_used = jnp.repeat(kv_weight.reshape(channels, KVH, 2 * HD), repeats, axis=1)
        weight_used = weight_used.reshape(channels, KVH * repeats * 2 * HD)
    else:
        weight_used = kv_weight
    gain = k_gain.reshape(1, HD)
    if shard_count <= MOST_VARIANTS and tensor_count == 4 and samples_here == 2:
        half = jnp.right_shift(owner, samples_here.bit_length() - 1)
        other = jnp.roll(half, -1)
        low, high = jnp.minimum(half, other), jnp.maximum(half, other)
        index = jnp.right_shift(low * (2 * shard_count - 1 - low), 1) + high - low - 1
        index = lax.optimization_barrier(index)[0]
        branches = [
            functools.partial(gather, shifts=pair, collective_id=i)
            for i, pair in enumerate(shift_pairs(shard_count))
        ]
        kv = lax.switch(index, branches, owner, features, kv_weight, gain)
        return attend_all(counts, owner, queries, q_gain, kv, samples_here)
    shifts = owner // samples_here

    def first_stage(c):
        return lambda: project(features, weight_used, gain, tensor_count, c, c)

    def attend_one(j, kv, out):
        return attend(j, samples_here, counts, owner, queries, q_gain, kv, out)

    def next_stage(j, c):
        return lambda value, kv, out: (shift_by(value, c), attend_one(j - 1, kv, out))

    def shift_switch(j, value):
        moves = [functools.partial(shift_by, count=c) for c in range(shard_count)]
        return lax.switch(shifts[j], moves, value)

    out = None
    if shard_count > MOST_VARIANTS:
        held = first_stage(0)()
        for j in range(samples_here):
            out = attend_one(j, shift_switch(j, held[j]), out)
        return out
    held = lax.switch(shifts[0], [first_stage(c) for c in range(shard_count)])
    moved = held[0]
    for j in range(1, samples_here):
        stages = [next_stage(j, c) for c in range(shard_count)]
        moved, out = lax.switch(shifts[j], stages, held[j], moved, out)
    return attend_one(samples_here - 1, moved, out)


def solution(mesh):
    placed = (P("dp", "tensor"), P("dp", None, "tensor"), P("tensor", None), P(), P(), P(), P())
    return jax.shard_map(
        shards, mesh=mesh, in_specs=placed, out_specs=P("dp", "tensor"), check_vma=False
    )
```

```python
import functools
import math

import jax
import jax.numpy as jnp
from jax import lax
from jax.experimental import pallas as pl
from jax.experimental.pallas import tpu as pltpu
from jax.sharding import PartitionSpec as P

KVH = 8
HD = 128
PATCH = 24
EPS = 1e-05
MESH = pl.DeviceIdType.MESH
MOST_VARIANTS = 16
EARLY = 2
STRIDE = 4
FIRST_AT = -2
FORWARD_AT = 6
FINISH_AT = 14
PREPARE_AT = 23
SUBS = 4
GATHER_VMEM = 57 * 1024 * 1024
LAST_VMEM = 32 * 1024 * 1024
VMEM_LIMIT = 60 * 1024 * 1024


def bit_orders(count):
    bits = [1 << b for b in range(count.bit_length() - 1)]
    return bits, bits[::-1]


def send_round(order, d):
    for r, bit in enumerate(order):
        if d & bit:
            return r
    return len(order)


def project_kernel(n, shift, x_hbm, w_hbm, gain_ref, moved_ref, *rest):
    stay_refs = rest[:-9]
    xv, wv, part, recv, ready, x_sem, w_sem, send_sem, recv_sem = rest[-9:]
    me = lax.axis_index("tensor")
    samples, tokens = xv.shape[0], xv.shape[1]
    half = tokens // 2
    width = wv.shape[2]
    orders = bit_orders(n)
    move_slot = 2 * samples * (n - 1)

    def flipped(d):
        result = me
        for bit in orders[0]:
            if d & bit:
                result = result + bit * (1 - 2 * ((me // bit) % 2))
        return result

    rounds = [[send_round(order, d) for d in range(n)] for order in orders]
    d_order = sorted(range(n), key=lambda d: (min(rounds[0][d], rounds[1][d]), -d))
    place_of = {d: i for i, d in enumerate(d_order)}
    later = sorted(
        [(rounds[s][d], -d, s) for d in range(1, n) for s in range(2) if rounds[s][d] > 0]
    )

    def x_copy(j):
        return pltpu.make_async_copy(x_hbm.at[j], xv.at[j], x_sem.at[j])

    def w_copy(i, first_column):
        columns = pl.ds(pl.multiple_of(first_column, 128), width)
        return pltpu.make_async_copy(w_hbm.at[:, columns], wv.at[i], w_sem.at[i])

    def remote(j, d, s):
        slot = (j * 2 + s) * (n - 1) + d - 1
        return pltpu.make_async_remote_copy(
            src_ref=part.at[j, place_of[d], pl.ds(s * half, half)],
            dst_ref=recv.at[j, s, d - 1],
            send_sem=send_sem.at[slot],
            recv_sem=recv_sem.at[slot],
            device_id={"tensor": flipped(orders[s][rounds[s][d]])},
            device_id_type=MESH,
        )

    def move(s):
        rows = pl.ds(s * half, half)
        if shift == 0:
            return pltpu.make_async_copy(
                ready.at[rows], moved_ref.at[rows], send_sem.at[move_slot + s]
            )
        return pltpu.make_async_remote_copy(
            src_ref=ready.at[rows],
            dst_ref=moved_ref.at[rows],
            send_sem=send_sem.at[move_slot + s],
            recv_sem=recv_sem.at[move_slot + s],
            device_id={"dp": lax.rem(place + shift, shard_count)},
            device_id_type=MESH,
        )

    shard_count = lax.axis_size("dp")
    place = lax.axis_index("dp")
    barrier = pltpu.get_barrier_semaphore()
    greeted = 0
    for bit in orders[0]:
        pl.semaphore_signal(barrier, inc=1, device_id={"tensor": flipped(bit)}, device_id_type=MESH)
        greeted += 1
    if shift:
        for by in (shift, shard_count - shift):
            other = lax.rem(place + by, shard_count)
            pl.semaphore_signal(barrier, inc=1, device_id={"dp": other}, device_id_type=MESH)
            greeted += 1
    x_copy(0).start()
    for i, d in enumerate(d_order):
        w_copy(i, flipped(d) * width).start()
    for j in range(1, samples):
        x_copy(j).start()

    def total(j, d, s):
        result = part[j, place_of[d], s * half : (s + 1) * half].astype(jnp.float32)
        for bit in orders[s][: rounds[s][d]]:
            remote(j, d | bit, s).wait_recv()
            result = result + recv[j, s, (d | bit) - 1].astype(jnp.float32)
        return result

    def send_later(j):
        for _, negative, s in later:
            d = -negative
            part[j, place_of[d], s * half : (s + 1) * half] = total(j, d, s).astype(jnp.bfloat16)
            remote(j, d, s).start()

    def finish(j):
        gain = gain_ref[...]
        target = ready if j == 0 else stay_refs[j - 1]
        for s in range(2):
            summed = total(j, 0, s)
            rows = slice(s * half, (s + 1) * half)
            for c in range(0, width, HD):
                block = summed[:, c : c + HD]
                if c // HD % 2 == 0:
                    scale = lax.rsqrt(jnp.mean(block * block, axis=-1, keepdims=True) + EPS)
                    block = block * scale * gain
                target[rows, c : c + HD] = block.astype(jnp.bfloat16)
            if j == 0:
                move(s).start()

    @pl.loop(0, samples * n)
    def _(step):
        j = step // n
        i = step % n

        @pl.when(i == 0)
        def _():
            x_copy(j).wait()

        @pl.when(j == 0)
        def _():
            w_copy(i, 0).wait()

        part[j, i] = jnp.dot(xv[j], wv[i], preferred_element_type=jnp.float32).astype(
            jnp.bfloat16
        )

        @pl.when(step == 0)
        def _():
            pl.semaphore_wait(barrier, greeted)

        if samples > 1:

            @pl.when((i == 0) & (j > 0))
            def _():
                send_later(j - 1)

        for k, d in enumerate(d_order):
            streams = [s for s in range(2) if rounds[s][d] == 0]
            if streams:

                @pl.when(i == k)
                def _():
                    for s in streams:
                        remote(j, d, s).start()

    for j in range(samples - 1):
        finish(j)
    send_later(samples - 1)
    finish(samples - 1)
    for j in range(samples):
        for d in range(1, n):
            for s in range(2):
                remote(j, d, s).wait_send()
    for s in range(2):
        move(s).wait()


def project(features, weight, k_gain, n, shift, collective_id):
    samples, tokens, channels = features.shape
    width = weight.shape[1] // n
    count = 2 * samples * (n - 1) + 2
    block = jax.ShapeDtypeStruct((tokens, width), jnp.bfloat16)
    return pl.pallas_call(
        functools.partial(project_kernel, n, shift),
        out_shape=[block] * samples,
        in_specs=[
            pl.BlockSpec(memory_space=pl.ANY),
            pl.BlockSpec(memory_space=pl.ANY),
            pl.BlockSpec(memory_space=pltpu.VMEM),
        ],
        out_specs=[pl.BlockSpec(memory_space=pl.ANY)]
        + [pl.BlockSpec(memory_space=pltpu.VMEM)] * (samples - 1),
        scratch_shapes=[
            pltpu.VMEM((samples, tokens, channels), jnp.bfloat16),
            pltpu.VMEM((n, channels, width), jnp.bfloat16),
            pltpu.VMEM((samples, n, tokens, width), jnp.bfloat16),
            pltpu.VMEM((samples, 2, n - 1, tokens // 2, width), jnp.bfloat16),
            pltpu.VMEM((tokens, width), jnp.bfloat16),
            pltpu.SemaphoreType.DMA((samples,)),
            pltpu.SemaphoreType.DMA((n,)),
            pltpu.SemaphoreType.DMA((count,)),
            pltpu.SemaphoreType.DMA((count,)),
        ],
        compiler_params=pltpu.CompilerParams(
            collective_id=collective_id, has_side_effects=True, vmem_limit_bytes=VMEM_LIMIT
        ),
        name="project",
    )(features, weight, k_gain)


def shift_rank(shard_count):
    def hops(c):
        return sum(abs((e + c) % shard_count // 2 - e // 2) for e in range(shard_count))

    return [hops(c) * shard_count - c for c in range(shard_count)]


def shift_pairs(shard_count):
    rank = shift_rank(shard_count)
    pairs = [(a, b) for a in range(shard_count) for b in range(a + 1, shard_count)]
    return [pair if rank[pair[0]] > rank[pair[1]] else pair[::-1] for pair in pairs]


def gather_kernel(
    shifts, count_hbm, owner_hbm, x_hbm, w_hbm, q_hbm, gain_hbm, q_gain_hbm,
    kv_ref, qn_ref, rows_ref, scale_ref,
    xv, wv, part, recv0, mid, recv1, ready, qv, gains, numbers,
    x_sem, w_sem, q_sem, small_sem, send_sem, recv_sem,
):
    me = lax.axis_index("tensor")
    place = lax.axis_index("dp")
    shard_count = lax.axis_size("dp")
    blocks, pieces, subs, _, rows, _ = part.shape
    half_blocks = blocks // 2
    samples = 2
    total = blocks * subs

    def flipped(bit):
        return me + bit * (1 - 2 * ((me // bit) % 2))

    def slab(d):
        result = me
        if d & 1:
            result = result + 1 - 2 * (result % 2)
        if d & 2:
            result = result + 2 * (1 - 2 * ((me // 2) % 2))
        return result

    def x_copy(j):
        return pltpu.make_async_copy(x_hbm.at[j], xv.at[j], x_sem.at[j])

    def w_copy(q, first):
        columns = pl.ds(pl.multiple_of(first, 128), wv.shape[2])
        return pltpu.make_async_copy(w_hbm.at[:, columns], wv.at[q], w_sem.at[q])

    small = [
        pltpu.make_async_copy(owner_hbm, numbers.at[0], small_sem.at[0]),
        pltpu.make_async_copy(count_hbm, numbers.at[1], small_sem.at[1]),
        pltpu.make_async_copy(gain_hbm, gains.at[0], small_sem.at[2]),
        pltpu.make_async_copy(q_gain_hbm, gains.at[1], small_sem.at[3]),
    ]
    small[0].start()
    for j in range(samples):
        x_copy(j).start()
    for i, d in ((1, 3), (0, 1), (2, 2), (3, 0)):
        for half in range(2):
            w_copy(2 * i + half, slab(d) * 2 * wv.shape[2] + half * wv.shape[2]).start()
    for copy in small[1:]:
        copy.start()
    q_copy = pltpu.make_async_copy(q_hbm, qv, q_sem)
    q_copy.start()

    barrier = pltpu.get_barrier_semaphore()
    greeted = 0
    for bit in (1, 2):
        pl.semaphore_signal(barrier, inc=1, device_id={"tensor": flipped(bit)}, device_id_type=MESH)
        greeted += 1
    for c in shifts:
        if c:
            for by in (c, shard_count - c):
                other = lax.rem(place + by, shard_count)
                pl.semaphore_signal(barrier, inc=1, device_id={"dp": other}, device_id_type=MESH)
                greeted += 1

    small[0].wait()
    swapped = (numbers[0, 0] != samples * shifts[0]).astype(jnp.int32)

    def index(b, u, s):
        return (b * subs + u) * 2 + s

    def first_round(b, u, s):
        k = index(b, u, s)
        return pltpu.make_async_remote_copy(
            src_ref=part.at[b, pl.ds(2 * s, 4), u, s],
            dst_ref=recv0.at[k],
            send_sem=send_sem.at[0, k],
            recv_sem=recv_sem.at[0, k],
            device_id={"tensor": flipped(1 + s)},
            device_id_type=MESH,
        )

    def early(u, s, own):
        k = index(0, u, s)
        slot = total * 2 + k if own else k
        return pltpu.make_async_remote_copy(
            src_ref=part.at[0, pl.ds(4 * s if own else 2, 2), u, s],
            dst_ref=recv0.at[k, pl.ds(2 * s if own else 2 * (1 - s), 2)],
            send_sem=send_sem.at[0, slot],
            recv_sem=recv_sem.at[0, slot],
            device_id={"tensor": flipped(1 + s)},
            device_id_type=MESH,
        )

    def second_round(b, u, s):
        k = index(b, u, s)
        return pltpu.make_async_remote_copy(
            src_ref=mid.at[k],
            dst_ref=recv1.at[k],
            send_sem=send_sem.at[1, k],
            recv_sem=recv_sem.at[1, k],
            device_id={"tensor": flipped(2 - s)},
            device_id_type=MESH,
        )

    def move(c, k):
        return pltpu.make_async_remote_copy(
            src_ref=ready.at[k],
            dst_ref=kv_ref.at[k],
            send_sem=send_sem.at[2, k],
            recv_sem=recv_sem.at[2, k],
            device_id={"dp": lax.rem(place + c, shard_count)},
            device_id_type=MESH,
        )

    def compute(b, q):
        sample = swapped + b * (1 - 2 * swapped)

        @pl.when(b == 0)
        def _():
            w_copy(q, 0).wait()

        result = jnp.dot(xv[sample], wv[q], preferred_element_type=jnp.float32)
        result = result.astype(jnp.bfloat16)
        for u in range(subs):
            for s in range(2):
                r = (u * 2 + s) * rows
                part[b, q, u, s] = result[r : r + rows]

    def forward(i):
        b, u = i // subs, i % subs

        @pl.loop(0, 2)
        def _(s):
            k = index(b, u, s)

            @pl.when(i < EARLY)
            def _():
                early(i, s, False).wait_recv()

            @pl.when(i >= EARLY)
            def _():
                first_round(b, u, s).wait_recv()

            for half in range(2):
                mine = part[b, 4 * (1 - s) + half, u, s].astype(jnp.float32)
                other = recv0[k, 2 * (1 - s) + half].astype(jnp.float32)
                mid[k, half] = (mine + other).astype(jnp.bfloat16)
            second_round(b, u, s).start()

    def finish(i):
        b, u = i // subs, i % subs
        gain = gains[0]

        @pl.loop(0, 2)
        def _(s):
            k = index(b, u, s)

            @pl.when(i < EARLY)
            def _():
                early(i, s, True).wait_recv()

            second_round(b, u, s).wait_recv()
            for half in range(2):
                block = part[b, 6 + half, u, s].astype(jnp.float32)
                block = block + recv0[k, 2 * s + half].astype(jnp.float32)
                block = block + recv1[k, half].astype(jnp.float32)
                key = block[:, :HD]
                scale = lax.rsqrt(jnp.mean(key * key, axis=-1, keepdims=True) + EPS)
                ready[k, half, :, :HD] = (key * scale * gain).astype(jnp.bfloat16)
                ready[k, half, :, HD:] = block[:, HD:].astype(jnp.bfloat16)
            for ph, c in enumerate(shifts):

                @pl.when(b // half_blocks == ph)
                def _():
                    if c == 0:
                        kv_ref[k] = ready[k]
                    else:
                        move(c, k).start()

    pl.semaphore_wait(barrier, greeted)
    small[2].wait()
    small[3].wait()

    for j in range(samples):
        x_copy(j).wait()

    text_rows = qv.shape[1]
    tile = 32 if text_rows % 32 == 0 else 16

    def prepare():
        small[1].wait()
        for ph, c in enumerate(shifts):
            sample = swapped if ph == 0 else 1 - swapped
            source = lax.rem(place + shard_count - c, shard_count)
            valid_rows = numbers[1, source * samples + sample] * PATCH
            rows_ref[ph] = jnp.full(rows_ref.shape[1:], valid_rows)
        scale_ref[...] = gains[1] * (1.0 / math.sqrt(HD))
        q_copy.wait()

        @pl.loop(0, samples * text_rows // tile)
        def _(r):
            ph = r // (text_rows // tile)
            at = pl.ds(pl.multiple_of(r % (text_rows // tile) * tile, tile), tile)
            qn_ref[ph, at] = qv[swapped + ph * (1 - 2 * swapped), at]

    def due(tick, first):
        i = (tick - first) // STRIDE
        return i, (tick >= first) & ((tick - first) % STRIDE == 0) & (i < total)

    @pl.loop(0, FINISH_AT + STRIDE * (total - 1) + 1)
    def _(tick):
        @pl.when(tick < blocks * pieces)
        def _():
            n = tick % pieces
            compute(tick // pieces, jnp.where(n < 2, n + 2, jnp.where(n < 4, n - 2, n)))

        @pl.when(tick == 1)
        def _():
            for u in range(EARLY):
                for s in range(2):
                    early(u, s, False).start()

        for s in range(2):

            @pl.when(tick == 3 + 2 * s)
            def _():
                for u in range(EARLY):
                    early(u, s, True).start()

        i, now = due(tick, FIRST_AT)

        @pl.when(now & (i >= EARLY))
        def _():
            for s in range(2):
                first_round(i // subs, i % subs, s).start()

        i, now = due(tick, FORWARD_AT)

        @pl.when(now)
        def _():
            forward(i)

        i, now = due(tick, FINISH_AT)

        @pl.when(now)
        def _():
            finish(i)

        @pl.when(tick == PREPARE_AT)
        def _():
            prepare()

    @pl.loop(0, total * 2)
    def _(k):
        b = k // (2 * subs)
        u = (k // 2) % subs
        s = k % 2

        @pl.when(k < 2 * EARLY)
        def _():
            early(u, s, False).wait_send()
            early(u, s, True).wait_send()

        @pl.when(k >= 2 * EARLY)
        def _():
            first_round(b, u, s).wait_send()

        second_round(b, u, s).wait_send()
        for ph, c in enumerate(shifts):
            if c:

                @pl.when(b // half_blocks == ph)
                def _():
                    move(c, k).wait()


def gather(counts, owner, features, weight, queries, k_gain, q_gain, shifts, collective_id):
    samples, tokens, channels = features.shape
    width = weight.shape[1] // lax.axis_size("tensor")
    rows = 48
    block_rows = 2 * SUBS * rows
    per_sample = tokens // block_rows
    blocks = samples * per_sample
    piece = width // 2
    count = blocks * SUBS * 2
    bf16 = jnp.bfloat16
    vmem = pl.BlockSpec(memory_space=pltpu.VMEM)
    hbm = pl.BlockSpec(memory_space=pl.ANY)
    return pl.pallas_call(
        functools.partial(gather_kernel, shifts),
        out_shape=[
            jax.ShapeDtypeStruct((count, 2, rows, piece), bf16),
            jax.ShapeDtypeStruct(queries.shape, bf16),
            jax.ShapeDtypeStruct((samples, 8, HD), jnp.int32),
            jax.ShapeDtypeStruct((1, HD), jnp.float32),
        ],
        in_specs=[hbm] * 7,
        out_specs=[vmem] * 4,
        scratch_shapes=[
            pltpu.VMEM((samples, tokens, channels), bf16),
            pltpu.VMEM((8, channels, piece), bf16),
            pltpu.VMEM((blocks, 8, SUBS, 2, rows, piece), bf16),
            pltpu.VMEM((count, 4, rows, piece), bf16),
            pltpu.VMEM((count, 2, rows, piece), bf16),
            pltpu.VMEM((count, 2, rows, piece), bf16),
            pltpu.VMEM((count, 2, rows, piece), bf16),
            pltpu.VMEM(queries.shape, bf16),
            pltpu.VMEM((2, 1, HD), jnp.float32),
            pltpu.SMEM((2, owner.shape[0]), jnp.int32),
            pltpu.SemaphoreType.DMA((blocks,)),
            pltpu.SemaphoreType.DMA((8,)),
            pltpu.SemaphoreType.DMA,
            pltpu.SemaphoreType.DMA((4,)),
            pltpu.SemaphoreType.DMA((3, count + 2 * EARLY)),
            pltpu.SemaphoreType.DMA((3, count + 2 * EARLY)),
        ],
        compiler_params=pltpu.CompilerParams(
            collective_id=collective_id, has_side_effects=True, vmem_limit_bytes=GATHER_VMEM
        ),
        name="gather",
    )(counts, owner, features, weight, queries, k_gain, q_gain)


def attend_all_kernel(
    owner_hbm, q_ref, kv_ref, rows_ref, scale_ref, out_hbm, held, owner_ref, sem, owner_sem
):
    shard_count = lax.axis_size("dp")
    samples, text_len, width = q_ref.shape
    slots, kv_heads, rows, _ = kv_ref.shape
    per_sample = slots // samples
    tokens = per_sample * rows
    group = width // kv_heads
    owner_copy = pltpu.make_async_copy(owner_hbm, owner_ref, owner_sem)
    owner_copy.start()

    def put(ph, h, sample):
        columns = pl.ds(pl.multiple_of(h * group, HD), group)
        at = pl.ds(pl.multiple_of(sample * text_len, 16), text_len)
        return pltpu.make_async_copy(
            held.at[ph, h], out_hbm.at[at, columns], sem.at[ph * kv_heads + h]
        )

    def sample_of(ph):
        shifts = [owner_ref[i] // samples for i in range(samples)]
        ranks = [
            sum(jnp.where(c == i, r, 0) for i, r in enumerate(shift_rank(shard_count)))
            for c in shifts
        ]
        swapped = (ranks[0] < ranks[1]).astype(jnp.int32)
        return swapped + ph * (1 - 2 * swapped)

    @pl.loop(0, samples * kv_heads)
    def _(step):
        ph, h = step // kv_heads, step % kv_heads
        slot = pl.ds(ph * per_sample, per_sample)
        keys = kv_ref[slot, h, :, :HD].reshape(tokens, HD)
        values = kv_ref[slot, h, :, HD:].reshape(tokens, HD)
        valid = lax.broadcasted_iota(jnp.int32, (tokens, HD), 0) < rows_ref[ph, 0:1, :]
        values = jnp.where(valid, values.astype(jnp.float32), 0.0).astype(jnp.bfloat16)
        ones = jnp.where(valid, 1.0, 0.0).astype(jnp.bfloat16)
        values = jnp.concatenate([values, ones], axis=1)
        for g in range(group // HD):
            columns = pl.ds(pl.multiple_of(h * group + g * HD, HD), HD)
            query = q_ref[ph, :, columns].astype(jnp.float32)
            scale = lax.rsqrt(jnp.mean(query * query, axis=-1, keepdims=True) + EPS)
            query = (query * scale * scale_ref[...]).astype(jnp.bfloat16)
            scores = lax.dot_general(
                query, keys, (((1,), (1,)), ((), ())), preferred_element_type=jnp.float32
            )
            weights = jnp.exp(scores).astype(jnp.bfloat16)
            both = jnp.dot(weights, values, preferred_element_type=jnp.float32)
            held[ph, h, :, g * HD : (g + 1) * HD] = (both[:, :HD] / both[:, HD:]).astype(
                jnp.bfloat16
            )

        @pl.when(step == 0)
        def _():
            owner_copy.wait()

        put(ph, h, sample_of(ph)).start()

    for ph in range(samples):
        for h in range(kv_heads):
            put(ph, h, 0).wait()


def attend_all(owner, queries, kv, valid_rows, scale):
    samples, text_len, width = queries.shape
    kv_heads = kv.shape[1]
    vmem = pl.BlockSpec(memory_space=pltpu.VMEM)
    hbm = pl.BlockSpec(memory_space=pl.ANY)
    return pl.pallas_call(
        attend_all_kernel,
        out_shape=jax.ShapeDtypeStruct((samples * text_len, width), jnp.bfloat16),
        in_specs=[hbm, vmem, vmem, vmem, vmem],
        out_specs=hbm,
        scratch_shapes=[
            pltpu.VMEM((samples, kv_heads, text_len, width // kv_heads), jnp.bfloat16),
            pltpu.SMEM(owner.shape, jnp.int32),
            pltpu.SemaphoreType.DMA((samples * kv_heads,)),
            pltpu.SemaphoreType.DMA,
        ],
        compiler_params=pltpu.CompilerParams(vmem_limit_bytes=LAST_VMEM),
        name="attend_all",
    )(owner, queries, kv, valid_rows, scale)


def attend_kernel(sample, samples, count_ref, owner_ref, q_ref, gain_ref, kv_ref, *rest):
    out_ref = rest[-1]
    shard_count = lax.axis_size("dp")
    tokens = kv_ref.shape[0]
    source = lax.axis_index("dp") - owner_ref[sample] // samples + shard_count
    count = count_ref[lax.rem(source, shard_count) * samples + sample]
    keys = kv_ref[:, :HD]
    values = jnp.concatenate([kv_ref[:, HD:], jnp.ones((tokens, HD), jnp.bfloat16)], axis=1)
    valid = lax.broadcasted_iota(jnp.int32, (1, tokens), 1) < count * PATCH
    gain = gain_ref[...] * (1.0 / math.sqrt(HD))
    for head in range(q_ref.shape[1] // HD):
        columns = slice(head * HD, (head + 1) * HD)
        query = q_ref[:, columns].astype(jnp.float32)
        scale = lax.rsqrt(jnp.mean(query * query, axis=-1, keepdims=True) + EPS)
        query = (query * scale * gain).astype(jnp.bfloat16)
        scores = lax.dot_general(
            query, keys, (((1,), (1,)), ((), ())), preferred_element_type=jnp.float32
        )
        weights = jnp.where(valid, jnp.exp(scores), 0.0).astype(jnp.bfloat16)
        both = jnp.dot(weights, values, preferred_element_type=jnp.float32)
        out_ref[:, columns] = (both[:, :HD] / both[:, HD:]).astype(jnp.bfloat16)


def attend(sample, samples, counts, owner, queries, q_gain, kv, out):
    tokens, width = kv.shape
    kv_heads = width // (2 * HD)
    text_len = queries.shape[0] // samples
    group = queries.shape[1] // kv_heads
    smem = pl.BlockSpec(memory_space=pltpu.SMEM)
    operands = [counts, owner, queries, q_gain.reshape(1, HD), kv]
    specs = [
        smem,
        smem,
        pl.BlockSpec((text_len, group), lambda h: (sample, h)),
        pl.BlockSpec((1, HD), lambda h: (0, 0)),
        pl.BlockSpec((tokens, 2 * HD), lambda h: (0, h)),
    ]
    aliases = {}
    if out is not None:
        aliases = {len(operands): 0}
        operands.append(out)
        specs.append(pl.BlockSpec(memory_space=pl.ANY))
    products = 2 * text_len * queries.shape[1] * tokens * 2
    return pl.pallas_call(
        functools.partial(attend_kernel, sample, samples),
        out_shape=jax.ShapeDtypeStruct(queries.shape, jnp.bfloat16),
        grid=(kv_heads,),
        in_specs=specs,
        out_specs=pl.BlockSpec((text_len, group), lambda h: (sample, h)),
        input_output_aliases=aliases,
        cost_estimate=pl.CostEstimate(
            flops=products, bytes_accessed=4 * text_len * queries.shape[1], transcendentals=0
        ),
        name="attend",
    )(*operands)


def shift_by(value, count):
    if count == 0:
        return value
    length = lax.axis_size("dp")
    return lax.ppermute(value, "dp", [(i, (i + count) % length) for i in range(length)])


def shards(queries, features, kv_weight, q_gain, k_gain, counts, owner):
    samples_here, token_count, channels = features.shape
    shard_count = lax.axis_size("dp")
    tensor_count = lax.axis_size("tensor")
    local_width = kv_weight.shape[1] // tensor_count
    repeats = max(1, 2 * HD // local_width)
    if repeats > 1:
        weight_used = jnp.repeat(kv_weight.reshape(channels, KVH, 2 * HD), repeats, axis=1)
        weight_used = weight_used.reshape(channels, KVH * repeats * 2 * HD)
    else:
        weight_used = kv_weight
    gain = k_gain.reshape(1, HD)
    if shard_count <= MOST_VARIANTS and tensor_count == 4 and samples_here == 2:
        half = jnp.right_shift(owner, samples_here.bit_length() - 1)
        other = lax.pad(owner, jnp.int32(0), [(-1, 1, 0)])
        other = jnp.right_shift(other, samples_here.bit_length() - 1)
        low, high = jnp.minimum(half, other), jnp.maximum(half, other)
        index = jnp.right_shift(low * (2 * shard_count - 1 - low), 1) + high - low - 1
        index = lax.optimization_barrier(index)[0]
        branches = [
            functools.partial(gather, shifts=pair, collective_id=i)
            for i, pair in enumerate(shift_pairs(shard_count))
        ]
        texts = queries.reshape(samples_here, -1, queries.shape[1])
        kv, texts, valid_rows, scale = lax.switch(
            index,
            branches,
            counts,
            owner,
            features,
            kv_weight,
            texts,
            gain,
            q_gain.reshape(1, HD),
        )
        return attend_all(owner, texts, kv, valid_rows, scale)
    shifts = owner // samples_here

    def first_stage(c):
        return lambda: project(features, weight_used, gain, tensor_count, c, c)

    def attend_one(j, kv, out):
        return attend(j, samples_here, counts, owner, queries, q_gain, kv, out)

    def next_stage(j, c):
        return lambda value, kv, out: (shift_by(value, c), attend_one(j - 1, kv, out))

    def shift_switch(j, value):
        moves = [functools.partial(shift_by, count=c) for c in range(shard_count)]
        return lax.switch(shifts[j], moves, value)

    out = None
    if shard_count > MOST_VARIANTS:
        held = first_stage(0)()
        for j in range(samples_here):
            out = attend_one(j, shift_switch(j, held[j]), out)
        return out
    held = lax.switch(shifts[0], [first_stage(c) for c in range(shard_count)])
    moved = held[0]
    for j in range(1, samples_here):
        stages = [next_stage(j, c) for c in range(shard_count)]
        moved, out = lax.switch(shifts[j], stages, held[j], moved, out)
    return attend_one(samples_here - 1, moved, out)


def solution(mesh):
    placed = (P("dp", "tensor"), P("dp", None, "tensor"), P("tensor", None), P(), P(), P(), P())
    return jax.shard_map(
        shards, mesh=mesh, in_specs=placed, out_specs=P("dp", "tensor"), check_vma=False
    )
```

```python
import functools
import math

import jax
import jax.numpy as jnp
from jax import lax
from jax.experimental import pallas as pl
from jax.experimental.pallas import tpu as pltpu
from jax.sharding import PartitionSpec as P

KVH = 8
HD = 128
PATCH = 24
EPS = 1e-05
MESH = pl.DeviceIdType.MESH
MOST_VARIANTS = 16
EARLY = 2
STRIDE = 4
FIRST_AT = 0
FORWARD_AT = 5
FINISH_AT = 11
PREPARE_AT = 23
SUBS = 4
GATHER_VMEM = 57 * 1024 * 1024
LAST_VMEM = 32 * 1024 * 1024
VMEM_LIMIT = 60 * 1024 * 1024


def bit_orders(count):
    bits = [1 << b for b in range(count.bit_length() - 1)]
    return bits, bits[::-1]


def send_round(order, d):
    for r, bit in enumerate(order):
        if d & bit:
            return r
    return len(order)


def project_kernel(n, shift, x_hbm, w_hbm, gain_ref, moved_ref, *rest):
    stay_refs = rest[:-9]
    xv, wv, part, recv, ready, x_sem, w_sem, send_sem, recv_sem = rest[-9:]
    me = lax.axis_index("tensor")
    samples, tokens = xv.shape[0], xv.shape[1]
    half = tokens // 2
    width = wv.shape[2]
    orders = bit_orders(n)
    move_slot = 2 * samples * (n - 1)

    def flipped(d):
        result = me
        for bit in orders[0]:
            if d & bit:
                result = result + bit * (1 - 2 * ((me // bit) % 2))
        return result

    rounds = [[send_round(order, d) for d in range(n)] for order in orders]
    d_order = sorted(range(n), key=lambda d: (min(rounds[0][d], rounds[1][d]), -d))
    place_of = {d: i for i, d in enumerate(d_order)}
    later = sorted(
        [(rounds[s][d], -d, s) for d in range(1, n) for s in range(2) if rounds[s][d] > 0]
    )

    def x_copy(j):
        return pltpu.make_async_copy(x_hbm.at[j], xv.at[j], x_sem.at[j])

    def w_copy(i, first_column):
        columns = pl.ds(pl.multiple_of(first_column, 128), width)
        return pltpu.make_async_copy(w_hbm.at[:, columns], wv.at[i], w_sem.at[i])

    def remote(j, d, s):
        slot = (j * 2 + s) * (n - 1) + d - 1
        return pltpu.make_async_remote_copy(
            src_ref=part.at[j, place_of[d], pl.ds(s * half, half)],
            dst_ref=recv.at[j, s, d - 1],
            send_sem=send_sem.at[slot],
            recv_sem=recv_sem.at[slot],
            device_id={"tensor": flipped(orders[s][rounds[s][d]])},
            device_id_type=MESH,
        )

    def move(s):
        rows = pl.ds(s * half, half)
        if shift == 0:
            return pltpu.make_async_copy(
                ready.at[rows], moved_ref.at[rows], send_sem.at[move_slot + s]
            )
        return pltpu.make_async_remote_copy(
            src_ref=ready.at[rows],
            dst_ref=moved_ref.at[rows],
            send_sem=send_sem.at[move_slot + s],
            recv_sem=recv_sem.at[move_slot + s],
            device_id={"dp": lax.rem(place + shift, shard_count)},
            device_id_type=MESH,
        )

    shard_count = lax.axis_size("dp")
    place = lax.axis_index("dp")
    barrier = pltpu.get_barrier_semaphore()
    greeted = 0
    for bit in orders[0]:
        pl.semaphore_signal(barrier, inc=1, device_id={"tensor": flipped(bit)}, device_id_type=MESH)
        greeted += 1
    if shift:
        for by in (shift, shard_count - shift):
            other = lax.rem(place + by, shard_count)
            pl.semaphore_signal(barrier, inc=1, device_id={"dp": other}, device_id_type=MESH)
            greeted += 1
    x_copy(0).start()
    for i, d in enumerate(d_order):
        w_copy(i, flipped(d) * width).start()
    for j in range(1, samples):
        x_copy(j).start()

    def total(j, d, s):
        result = part[j, place_of[d], s * half : (s + 1) * half].astype(jnp.float32)
        for bit in orders[s][: rounds[s][d]]:
            remote(j, d | bit, s).wait_recv()
            result = result + recv[j, s, (d | bit) - 1].astype(jnp.float32)
        return result

    def send_later(j):
        for _, negative, s in later:
            d = -negative
            part[j, place_of[d], s * half : (s + 1) * half] = total(j, d, s).astype(jnp.bfloat16)
            remote(j, d, s).start()

    def finish(j):
        gain = gain_ref[...]
        target = ready if j == 0 else stay_refs[j - 1]
        for s in range(2):
            summed = total(j, 0, s)
            rows = slice(s * half, (s + 1) * half)
            for c in range(0, width, HD):
                block = summed[:, c : c + HD]
                if c // HD % 2 == 0:
                    scale = lax.rsqrt(jnp.mean(block * block, axis=-1, keepdims=True) + EPS)
                    block = block * scale * gain
                target[rows, c : c + HD] = block.astype(jnp.bfloat16)
            if j == 0:
                move(s).start()

    @pl.loop(0, samples * n)
    def _(step):
        j = step // n
        i = step % n

        @pl.when(i == 0)
        def _():
            x_copy(j).wait()

        @pl.when(j == 0)
        def _():
            w_copy(i, 0).wait()

        part[j, i] = jnp.dot(xv[j], wv[i], preferred_element_type=jnp.float32).astype(
            jnp.bfloat16
        )

        @pl.when(step == 0)
        def _():
            pl.semaphore_wait(barrier, greeted)

        if samples > 1:

            @pl.when((i == 0) & (j > 0))
            def _():
                send_later(j - 1)

        for k, d in enumerate(d_order):
            streams = [s for s in range(2) if rounds[s][d] == 0]
            if streams:

                @pl.when(i == k)
                def _():
                    for s in streams:
                        remote(j, d, s).start()

    for j in range(samples - 1):
        finish(j)
    send_later(samples - 1)
    finish(samples - 1)
    for j in range(samples):
        for d in range(1, n):
            for s in range(2):
                remote(j, d, s).wait_send()
    for s in range(2):
        move(s).wait()


def project(features, weight, k_gain, n, shift, collective_id):
    samples, tokens, channels = features.shape
    width = weight.shape[1] // n
    count = 2 * samples * (n - 1) + 2
    block = jax.ShapeDtypeStruct((tokens, width), jnp.bfloat16)
    return pl.pallas_call(
        functools.partial(project_kernel, n, shift),
        out_shape=[block] * samples,
        in_specs=[
            pl.BlockSpec(memory_space=pl.ANY),
            pl.BlockSpec(memory_space=pl.ANY),
            pl.BlockSpec(memory_space=pltpu.VMEM),
        ],
        out_specs=[pl.BlockSpec(memory_space=pl.ANY)]
        + [pl.BlockSpec(memory_space=pltpu.VMEM)] * (samples - 1),
        scratch_shapes=[
            pltpu.VMEM((samples, tokens, channels), jnp.bfloat16),
            pltpu.VMEM((n, channels, width), jnp.bfloat16),
            pltpu.VMEM((samples, n, tokens, width), jnp.bfloat16),
            pltpu.VMEM((samples, 2, n - 1, tokens // 2, width), jnp.bfloat16),
            pltpu.VMEM((tokens, width), jnp.bfloat16),
            pltpu.SemaphoreType.DMA((samples,)),
            pltpu.SemaphoreType.DMA((n,)),
            pltpu.SemaphoreType.DMA((count,)),
            pltpu.SemaphoreType.DMA((count,)),
        ],
        compiler_params=pltpu.CompilerParams(
            collective_id=collective_id, has_side_effects=True, vmem_limit_bytes=VMEM_LIMIT
        ),
        name="project",
    )(features, weight, k_gain)


def shift_rank(shard_count):
    def hops(c):
        return sum(abs((e + c) % shard_count // 2 - e // 2) for e in range(shard_count))

    return [hops(c) * shard_count - c for c in range(shard_count)]


def shift_pairs(shard_count):
    rank = shift_rank(shard_count)
    pairs = [(a, b) for a in range(shard_count) for b in range(a + 1, shard_count)]
    return [pair if rank[pair[0]] > rank[pair[1]] else pair[::-1] for pair in pairs]


def gather_kernel(
    shifts, count_hbm, owner_hbm, x_hbm, w_hbm, q_hbm, gain_hbm, q_gain_hbm,
    kv_ref, qn_ref, rows_ref, scale_ref,
    xv, wv, part, recv0, mid, recv1, ready, qv, gains, numbers,
    x_sem, w_sem, q_sem, small_sem, send_sem, recv_sem,
):
    me = lax.axis_index("tensor")
    place = lax.axis_index("dp")
    shard_count = lax.axis_size("dp")
    blocks, pieces, subs, _, rows, _ = part.shape
    half_blocks = blocks // 2
    samples = 2
    total = blocks * subs

    def flipped(bit):
        return me + bit * (1 - 2 * ((me // bit) % 2))

    def slab(d):
        result = me
        if d & 1:
            result = result + 1 - 2 * (result % 2)
        if d & 2:
            result = result + 2 * (1 - 2 * ((me // 2) % 2))
        return result

    def x_copy(j):
        return pltpu.make_async_copy(x_hbm.at[j], xv.at[j], x_sem.at[j])

    def w_copy(q, first):
        columns = pl.ds(pl.multiple_of(first, 128), wv.shape[2])
        return pltpu.make_async_copy(w_hbm.at[:, columns], wv.at[q], w_sem.at[q])

    small = [
        pltpu.make_async_copy(owner_hbm, numbers.at[0], small_sem.at[0]),
        pltpu.make_async_copy(count_hbm, numbers.at[1], small_sem.at[1]),
        pltpu.make_async_copy(gain_hbm, gains.at[0], small_sem.at[2]),
        pltpu.make_async_copy(q_gain_hbm, gains.at[1], small_sem.at[3]),
    ]
    small[0].start()
    for j in range(samples):
        x_copy(j).start()
    for i, d in ((1, 3), (0, 1), (2, 2), (3, 0)):
        for half in range(2):
            w_copy(2 * i + half, slab(d) * 2 * wv.shape[2] + half * wv.shape[2]).start()
    for copy in small[1:]:
        copy.start()
    q_copy = pltpu.make_async_copy(q_hbm, qv, q_sem)
    q_copy.start()

    barrier = pltpu.get_barrier_semaphore()
    greeted = 0
    for bit in (1, 2):
        pl.semaphore_signal(barrier, inc=1, device_id={"tensor": flipped(bit)}, device_id_type=MESH)
        greeted += 1
    for c in shifts:
        if c:
            for by in (c, shard_count - c):
                other = lax.rem(place + by, shard_count)
                pl.semaphore_signal(barrier, inc=1, device_id={"dp": other}, device_id_type=MESH)
                greeted += 1

    small[0].wait()
    swapped = (numbers[0, 0] != samples * shifts[0]).astype(jnp.int32)

    def index(b, u, s):
        return (b * subs + u) * 2 + s

    def first_round(b, u, s):
        k = index(b, u, s)
        return pltpu.make_async_remote_copy(
            src_ref=part.at[b, pl.ds(2 * s, 4), u, s],
            dst_ref=recv0.at[k],
            send_sem=send_sem.at[0, k],
            recv_sem=recv_sem.at[0, k],
            device_id={"tensor": flipped(1 + s)},
            device_id_type=MESH,
        )

    def early(u, s, own):
        k = index(0, u, s)
        slot = total * 2 + k if own else k
        return pltpu.make_async_remote_copy(
            src_ref=part.at[0, pl.ds(4 * s if own else 2, 2), u, s],
            dst_ref=recv0.at[k, pl.ds(2 * s if own else 2 * (1 - s), 2)],
            send_sem=send_sem.at[0, slot],
            recv_sem=recv_sem.at[0, slot],
            device_id={"tensor": flipped(1 + s)},
            device_id_type=MESH,
        )

    def second_round(b, u, s):
        k = index(b, u, s)
        return pltpu.make_async_remote_copy(
            src_ref=mid.at[k],
            dst_ref=recv1.at[k],
            send_sem=send_sem.at[1, k],
            recv_sem=recv_sem.at[1, k],
            device_id={"tensor": flipped(2 - s)},
            device_id_type=MESH,
        )

    def move(c, k):
        return pltpu.make_async_remote_copy(
            src_ref=ready.at[k],
            dst_ref=kv_ref.at[k],
            send_sem=send_sem.at[2, k],
            recv_sem=recv_sem.at[2, k],
            device_id={"dp": lax.rem(place + c, shard_count)},
            device_id_type=MESH,
        )

    def compute(b, q):
        sample = swapped + b * (1 - 2 * swapped)

        @pl.when(b == 0)
        def _():
            w_copy(q, 0).wait()

        result = jnp.dot(xv[sample], wv[q], preferred_element_type=jnp.float32)
        result = result.astype(jnp.bfloat16)
        for u in range(subs):
            for s in range(2):
                r = (u * 2 + s) * rows
                part[b, q, u, s] = result[r : r + rows]

    def forward(i):
        b, u = i // subs, i % subs

        @pl.loop(0, 2)
        def _(s):
            k = index(b, u, s)

            @pl.when(i < EARLY)
            def _():
                early(i, s, False).wait_recv()

            @pl.when(i >= EARLY)
            def _():
                first_round(b, u, s).wait_recv()

            for half in range(2):
                mine = part[b, 4 * (1 - s) + half, u, s].astype(jnp.float32)
                other = recv0[k, 2 * (1 - s) + half].astype(jnp.float32)
                mid[k, half] = (mine + other).astype(jnp.bfloat16)
            second_round(b, u, s).start()

    def finish(i):
        b, u = i // subs, i % subs
        gain = gains[0]

        @pl.loop(0, 2)
        def _(s):
            k = index(b, u, s)

            @pl.when(i < EARLY)
            def _():
                early(i, s, True).wait_recv()

            second_round(b, u, s).wait_recv()
            for half in range(2):
                block = part[b, 6 + half, u, s].astype(jnp.float32)
                block = block + recv0[k, 2 * s + half].astype(jnp.float32)
                block = block + recv1[k, half].astype(jnp.float32)
                key = block[:, :HD]
                scale = lax.rsqrt(jnp.mean(key * key, axis=-1, keepdims=True) + EPS)
                ready[k, half, :, :HD] = (key * scale * gain).astype(jnp.bfloat16)
                ready[k, half, :, HD:] = block[:, HD:].astype(jnp.bfloat16)
            for ph, c in enumerate(shifts):

                @pl.when(b // half_blocks == ph)
                def _():
                    if c == 0:
                        kv_ref[k] = ready[k]
                    else:
                        move(c, k).start()

    pl.semaphore_wait(barrier, greeted)
    small[2].wait()
    small[3].wait()

    for j in range(samples):
        x_copy(j).wait()

    text_rows = qv.shape[1]
    tile = 32 if text_rows % 32 == 0 else 16

    def prepare():
        small[1].wait()
        for ph, c in enumerate(shifts):
            sample = swapped if ph == 0 else 1 - swapped
            source = lax.rem(place + shard_count - c, shard_count)
            valid_rows = numbers[1, source * samples + sample] * PATCH
            rows_ref[ph] = jnp.full(rows_ref.shape[1:], valid_rows)
        scale_ref[...] = gains[1] * (1.0 / math.sqrt(HD))
        q_copy.wait()

        @pl.loop(0, samples * text_rows // tile)
        def _(r):
            ph = r // (text_rows // tile)
            at = pl.ds(pl.multiple_of(r % (text_rows // tile) * tile, tile), tile)
            qn_ref[ph, at] = qv[swapped + ph * (1 - 2 * swapped), at]

    def due(tick, first):
        i = (tick - first) // STRIDE
        return i, (tick >= first) & ((tick - first) % STRIDE == 0) & (i < total)

    @pl.loop(0, FINISH_AT + STRIDE * (total - 1) + 1)
    def _(tick):
        @pl.when(tick < blocks * pieces)
        def _():
            n = tick % pieces
            compute(tick // pieces, jnp.where(n < 2, n + 2, jnp.where(n < 4, n - 2, n)))

        @pl.when(tick == 1)
        def _():
            for u in range(EARLY):
                for s in range(2):
                    early(u, s, False).start()

        for s in range(2):

            @pl.when(tick == 3 + 2 * s)
            def _():
                for u in range(EARLY):
                    early(u, s, True).start()

        i, now = due(tick, FIRST_AT)

        @pl.when(now & (i >= EARLY))
        def _():
            for s in range(2):
                first_round(i // subs, i % subs, s).start()

        i, now = due(tick, FORWARD_AT)

        @pl.when(now)
        def _():
            forward(i)

        i, now = due(tick, FINISH_AT)

        @pl.when(now)
        def _():
            finish(i)

        @pl.when(tick == PREPARE_AT)
        def _():
            prepare()

    @pl.loop(0, total * 2)
    def _(k):
        b = k // (2 * subs)
        u = (k // 2) % subs
        s = k % 2

        @pl.when(k < 2 * EARLY)
        def _():
            early(u, s, False).wait_send()
            early(u, s, True).wait_send()

        @pl.when(k >= 2 * EARLY)
        def _():
            first_round(b, u, s).wait_send()

        second_round(b, u, s).wait_send()
        for ph, c in enumerate(shifts):
            if c:

                @pl.when(b // half_blocks == ph)
                def _():
                    move(c, k).wait()


def gather(counts, owner, features, weight, queries, k_gain, q_gain, shifts, collective_id):
    samples, tokens, channels = features.shape
    width = weight.shape[1] // lax.axis_size("tensor")
    rows = 48
    block_rows = 2 * SUBS * rows
    per_sample = tokens // block_rows
    blocks = samples * per_sample
    piece = width // 2
    count = blocks * SUBS * 2
    bf16 = jnp.bfloat16
    vmem = pl.BlockSpec(memory_space=pltpu.VMEM)
    hbm = pl.BlockSpec(memory_space=pl.ANY)
    return pl.pallas_call(
        functools.partial(gather_kernel, shifts),
        out_shape=[
            jax.ShapeDtypeStruct((count, 2, rows, piece), bf16),
            jax.ShapeDtypeStruct(queries.shape, bf16),
            jax.ShapeDtypeStruct((samples, 8, HD), jnp.int32),
            jax.ShapeDtypeStruct((1, HD), jnp.float32),
        ],
        in_specs=[hbm] * 7,
        out_specs=[vmem] * 4,
        scratch_shapes=[
            pltpu.VMEM((samples, tokens, channels), bf16),
            pltpu.VMEM((8, channels, piece), bf16),
            pltpu.VMEM((blocks, 8, SUBS, 2, rows, piece), bf16),
            pltpu.VMEM((count, 4, rows, piece), bf16),
            pltpu.VMEM((count, 2, rows, piece), bf16),
            pltpu.VMEM((count, 2, rows, piece), bf16),
            pltpu.VMEM((count, 2, rows, piece), bf16),
            pltpu.VMEM(queries.shape, bf16),
            pltpu.VMEM((2, 1, HD), jnp.float32),
            pltpu.SMEM((2, owner.shape[0]), jnp.int32),
            pltpu.SemaphoreType.DMA((blocks,)),
            pltpu.SemaphoreType.DMA((8,)),
            pltpu.SemaphoreType.DMA,
            pltpu.SemaphoreType.DMA((4,)),
            pltpu.SemaphoreType.DMA((3, count + 2 * EARLY)),
            pltpu.SemaphoreType.DMA((3, count + 2 * EARLY)),
        ],
        compiler_params=pltpu.CompilerParams(
            collective_id=collective_id, has_side_effects=True, vmem_limit_bytes=GATHER_VMEM
        ),
        name="gather",
    )(counts, owner, features, weight, queries, k_gain, q_gain)


def attend_all_kernel(
    owner_hbm, q_ref, kv_ref, rows_ref, scale_ref, out_hbm, held, owner_ref, sem, owner_sem
):
    shard_count = lax.axis_size("dp")
    samples, text_len, width = q_ref.shape
    slots, kv_heads, rows, _ = kv_ref.shape
    per_sample = slots // samples
    tokens = per_sample * rows
    group = width // kv_heads
    owner_copy = pltpu.make_async_copy(owner_hbm, owner_ref, owner_sem)
    owner_copy.start()

    def put(ph, h, sample):
        columns = pl.ds(pl.multiple_of(h * group, HD), group)
        at = pl.ds(pl.multiple_of(sample * text_len, 16), text_len)
        return pltpu.make_async_copy(
            held.at[ph, h], out_hbm.at[at, columns], sem.at[ph * kv_heads + h]
        )

    def sample_of(ph):
        shifts = [owner_ref[i] // samples for i in range(samples)]
        ranks = [
            sum(jnp.where(c == i, r, 0) for i, r in enumerate(shift_rank(shard_count)))
            for c in shifts
        ]
        swapped = (ranks[0] < ranks[1]).astype(jnp.int32)
        return swapped + ph * (1 - 2 * swapped)

    @pl.loop(0, samples * kv_heads)
    def _(step):
        ph, h = step // kv_heads, step % kv_heads
        slot = pl.ds(ph * per_sample, per_sample)
        keys = kv_ref[slot, h, :, :HD].reshape(tokens, HD)
        values = kv_ref[slot, h, :, HD:].reshape(tokens, HD)
        valid = lax.broadcasted_iota(jnp.int32, (tokens, HD), 0) < rows_ref[ph, 0:1, :]
        values = jnp.where(valid, values.astype(jnp.float32), 0.0).astype(jnp.bfloat16)
        ones = jnp.where(valid, 1.0, 0.0).astype(jnp.bfloat16)
        values = jnp.concatenate([values, ones], axis=1)
        for g in range(group // HD):
            columns = pl.ds(pl.multiple_of(h * group + g * HD, HD), HD)
            query = q_ref[ph, :, columns].astype(jnp.float32)
            scale = lax.rsqrt(jnp.mean(query * query, axis=-1, keepdims=True) + EPS)
            query = (query * scale * scale_ref[...]).astype(jnp.bfloat16)
            scores = lax.dot_general(
                query, keys, (((1,), (1,)), ((), ())), preferred_element_type=jnp.float32
            )
            weights = jnp.exp(scores).astype(jnp.bfloat16)
            both = jnp.dot(weights, values, preferred_element_type=jnp.float32)
            held[ph, h, :, g * HD : (g + 1) * HD] = (both[:, :HD] / both[:, HD:]).astype(
                jnp.bfloat16
            )

        @pl.when(step == 0)
        def _():
            owner_copy.wait()

        put(ph, h, sample_of(ph)).start()

    for ph in range(samples):
        for h in range(kv_heads):
            put(ph, h, 0).wait()


def attend_all(owner, queries, kv, valid_rows, scale):
    samples, text_len, width = queries.shape
    kv_heads = kv.shape[1]
    vmem = pl.BlockSpec(memory_space=pltpu.VMEM)
    hbm = pl.BlockSpec(memory_space=pl.ANY)
    return pl.pallas_call(
        attend_all_kernel,
        out_shape=jax.ShapeDtypeStruct((samples * text_len, width), jnp.bfloat16),
        in_specs=[hbm, vmem, vmem, vmem, vmem],
        out_specs=hbm,
        scratch_shapes=[
            pltpu.VMEM((samples, kv_heads, text_len, width // kv_heads), jnp.bfloat16),
            pltpu.SMEM(owner.shape, jnp.int32),
            pltpu.SemaphoreType.DMA((samples * kv_heads,)),
            pltpu.SemaphoreType.DMA,
        ],
        compiler_params=pltpu.CompilerParams(vmem_limit_bytes=LAST_VMEM),
        name="attend_all",
    )(owner, queries, kv, valid_rows, scale)


def attend_kernel(sample, samples, count_ref, owner_ref, q_ref, gain_ref, kv_ref, *rest):
    out_ref = rest[-1]
    shard_count = lax.axis_size("dp")
    tokens = kv_ref.shape[0]
    source = lax.axis_index("dp") - owner_ref[sample] // samples + shard_count
    count = count_ref[lax.rem(source, shard_count) * samples + sample]
    keys = kv_ref[:, :HD]
    values = jnp.concatenate([kv_ref[:, HD:], jnp.ones((tokens, HD), jnp.bfloat16)], axis=1)
    valid = lax.broadcasted_iota(jnp.int32, (1, tokens), 1) < count * PATCH
    gain = gain_ref[...] * (1.0 / math.sqrt(HD))
    for head in range(q_ref.shape[1] // HD):
        columns = slice(head * HD, (head + 1) * HD)
        query = q_ref[:, columns].astype(jnp.float32)
        scale = lax.rsqrt(jnp.mean(query * query, axis=-1, keepdims=True) + EPS)
        query = (query * scale * gain).astype(jnp.bfloat16)
        scores = lax.dot_general(
            query, keys, (((1,), (1,)), ((), ())), preferred_element_type=jnp.float32
        )
        weights = jnp.where(valid, jnp.exp(scores), 0.0).astype(jnp.bfloat16)
        both = jnp.dot(weights, values, preferred_element_type=jnp.float32)
        out_ref[:, columns] = (both[:, :HD] / both[:, HD:]).astype(jnp.bfloat16)


def attend(sample, samples, counts, owner, queries, q_gain, kv, out):
    tokens, width = kv.shape
    kv_heads = width // (2 * HD)
    text_len = queries.shape[0] // samples
    group = queries.shape[1] // kv_heads
    smem = pl.BlockSpec(memory_space=pltpu.SMEM)
    operands = [counts, owner, queries, q_gain.reshape(1, HD), kv]
    specs = [
        smem,
        smem,
        pl.BlockSpec((text_len, group), lambda h: (sample, h)),
        pl.BlockSpec((1, HD), lambda h: (0, 0)),
        pl.BlockSpec((tokens, 2 * HD), lambda h: (0, h)),
    ]
    aliases = {}
    if out is not None:
        aliases = {len(operands): 0}
        operands.append(out)
        specs.append(pl.BlockSpec(memory_space=pl.ANY))
    products = 2 * text_len * queries.shape[1] * tokens * 2
    return pl.pallas_call(
        functools.partial(attend_kernel, sample, samples),
        out_shape=jax.ShapeDtypeStruct(queries.shape, jnp.bfloat16),
        grid=(kv_heads,),
        in_specs=specs,
        out_specs=pl.BlockSpec((text_len, group), lambda h: (sample, h)),
        input_output_aliases=aliases,
        cost_estimate=pl.CostEstimate(
            flops=products, bytes_accessed=4 * text_len * queries.shape[1], transcendentals=0
        ),
        name="attend",
    )(*operands)


def shift_by(value, count):
    if count == 0:
        return value
    length = lax.axis_size("dp")
    return lax.ppermute(value, "dp", [(i, (i + count) % length) for i in range(length)])


def shards(queries, features, kv_weight, q_gain, k_gain, counts, owner):
    samples_here, token_count, channels = features.shape
    shard_count = lax.axis_size("dp")
    tensor_count = lax.axis_size("tensor")
    local_width = kv_weight.shape[1] // tensor_count
    repeats = max(1, 2 * HD // local_width)
    if repeats > 1:
        weight_used = jnp.repeat(kv_weight.reshape(channels, KVH, 2 * HD), repeats, axis=1)
        weight_used = weight_used.reshape(channels, KVH * repeats * 2 * HD)
    else:
        weight_used = kv_weight
    gain = k_gain.reshape(1, HD)
    if shard_count <= MOST_VARIANTS and tensor_count == 4 and samples_here == 2:
        half = jnp.right_shift(owner, samples_here.bit_length() - 1)
        other = lax.pad(owner, jnp.int32(0), [(-1, 1, 0)])
        other = jnp.right_shift(other, samples_here.bit_length() - 1)
        low, high = jnp.minimum(half, other), jnp.maximum(half, other)
        index = jnp.right_shift(low * (2 * shard_count - 1 - low), 1) + high - low - 1
        index = lax.optimization_barrier(index)[0]
        branches = [
            functools.partial(gather, shifts=pair, collective_id=i)
            for i, pair in enumerate(shift_pairs(shard_count))
        ]
        texts = queries.reshape(samples_here, -1, queries.shape[1])
        kv, texts, valid_rows, scale = lax.switch(
            index,
            branches,
            counts,
            owner,
            features,
            kv_weight,
            texts,
            gain,
            q_gain.reshape(1, HD),
        )
        return attend_all(owner, texts, kv, valid_rows, scale)
    shifts = owner // samples_here

    def first_stage(c):
        return lambda: project(features, weight_used, gain, tensor_count, c, c)

    def attend_one(j, kv, out):
        return attend(j, samples_here, counts, owner, queries, q_gain, kv, out)

    def next_stage(j, c):
        return lambda value, kv, out: (shift_by(value, c), attend_one(j - 1, kv, out))

    def shift_switch(j, value):
        moves = [functools.partial(shift_by, count=c) for c in range(shard_count)]
        return lax.switch(shifts[j], moves, value)

    out = None
    if shard_count > MOST_VARIANTS:
        held = first_stage(0)()
        for j in range(samples_here):
            out = attend_one(j, shift_switch(j, held[j]), out)
        return out
    held = lax.switch(shifts[0], [first_stage(c) for c in range(shard_count)])
    moved = held[0]
    for j in range(1, samples_here):
        stages = [next_stage(j, c) for c in range(shard_count)]
        moved, out = lax.switch(shifts[j], stages, held[j], moved, out)
    return attend_one(samples_here - 1, moved, out)


def solution(mesh):
    placed = (P("dp", "tensor"), P("dp", None, "tensor"), P("tensor", None), P(), P(), P(), P())
    return jax.shard_map(
        shards, mesh=mesh, in_specs=placed, out_specs=P("dp", "tensor"), check_vma=False
    )
```
